16 devices in a mesh: dp: 2 (over z), ep: 8 (over y, x, core).
Axes of the slice: x: 2, y: 2, z: 2, core: 2. Of those that a mesh axis runs over, the one named last changes fastest.
Arguments:
- hidden: bfloat16 [1024, 2048], P(('dp', 'ep')), parts along dimension 0
- positions: int32 [1024], P(('dp', 'ep')), parts along dimension 0
- expert_ids: int32 [2, 1024, 8], P(None, ('dp', 'ep')), parts along dimension 1
- k_cache: bfloat16 [2, 1024, 16, 16, 128], P(None, ('dp', 'ep')), parts along dimension 1
- v_cache: bfloat16 [2, 1024, 16, 16, 128], P(None, ('dp', 'ep')), parts along dimension 1
- w_query: bfloat16 [2, 2048, 2048], replicated
- w_key: bfloat16 [2, 2048, 2048], replicated
- w_value: bfloat16 [2, 2048, 2048], replicated
- w_out: bfloat16 [2, 2048, 2048], replicated
- attn_gain: float32 [2, 2048], replicated
- q_gain: float32 [2, 2048], replicated
- k_gain: float32 [2, 2048], replicated
- mlp_gain: float32 [2, 2048], replicated
- w_router: bfloat16 [2048, 64], replicated
- w_gate: bfloat16 [64, 2048, 1024], P('ep')
- w_up: bfloat16 [64, 2048, 1024], P('ep')
- w_down: bfloat16 [64, 1024, 2048], P('ep')
Outputs:
- output 1: bfloat16 [1024, 2048], P(('dp', 'ep')), parts along dimension 0
- output 2: bfloat16 [2, 1024, 16, 16, 128], P(None, ('dp', 'ep')), parts along dimension 1
- output 3: bfloat16 [2, 1024, 16, 16, 128], P(None, ('dp', 'ep')), parts along dimension 1
There are 2 independent parts. The reference program is written for one: setup_inputs(seed, part) draws one part's arguments, and reference() takes and returns one part's arrays. A program takes and returns all parts, laid end to end along the dimension named above; an argument that names none is the same for every part.
All inputs are finite; a program needn't handle non-finite values.
Results may differ from the reference program's by a relative error of at most 0.02.
Values are sent between devices in bfloat16 or wider.
A program may use at most 1 GiB of HBM per device.

```python
import jax
import jax.numpy as jnp
from jax import lax

SEQ_COUNT = 512
CACHE_LEN = 16
MODEL_DIM = 2048
NUM_HEADS = 16
KV_HEADS = 16
HEAD_DIM = 128
NUM_EXPERTS = 64
TOP_K = 8
FFN_DIM = 1024
EP_GROUPS = 8
NUM_LAYERS = 2

LOCAL_SEQS = SEQ_COUNT // EP_GROUPS
CAPACITY = 2 * LOCAL_SEQS * TOP_K // NUM_EXPERTS
WINDOWS = NUM_EXPERTS // TOP_K
Q_WIDTH = NUM_HEADS * HEAD_DIM
KV_WIDTH = KV_HEADS * HEAD_DIM
RMS_EPS = 1e-5
ROPE_BASE = 10000.0


def block_routes(rng_key):
    key_rows, key_perm = jax.random.split(rng_key)
    spread = jnp.arange(LOCAL_SEQS - CAPACITY, dtype=jnp.int32) % (WINDOWS - 1) + 1
    window_list = jnp.concatenate([jnp.zeros((CAPACITY,), jnp.int32), spread])
    windows = window_list[jax.random.permutation(key_rows, LOCAL_SEQS)]
    expert_perm = jax.random.permutation(key_perm, NUM_EXPERTS).astype(jnp.int32)
    slot_ids = windows[:, None] * TOP_K + jnp.arange(TOP_K, dtype=jnp.int32)[None, :]
    return expert_perm[slot_ids]


def draw_routes(rng_key):
    layer_keys = jax.random.split(rng_key, NUM_LAYERS * EP_GROUPS)
    routes = jax.vmap(block_routes)(layer_keys)
    return routes.reshape(NUM_LAYERS, SEQ_COUNT, TOP_K)


def draw_positions(rng_key):
    key_len, key_top = jax.random.split(rng_key)
    positions = jax.random.randint(key_len, (SEQ_COUNT,), 0, CACHE_LEN, dtype=jnp.int32)
    longest = jax.random.randint(key_top, (), 0, SEQ_COUNT)
    return positions.at[longest].set(CACHE_LEN - 1)


def setup_inputs(seed: int = 0, part: int = 0) -> dict:
    part_keys = jax.random.split(jax.random.fold_in(jax.random.key(seed + 1), part), 5)
    shared = jax.random.split(jax.random.key(seed), 12)

    def draw_normal(rng_key, shape, scale):
        return (jax.random.normal(rng_key, shape, jnp.float32) * scale).astype(jnp.bfloat16)

    def draw_gain(rng_key, shape):
        return 1.0 + 0.3 * jax.random.normal(rng_key, shape, jnp.float32)

    cache_shape = (NUM_LAYERS, SEQ_COUNT, CACHE_LEN, KV_HEADS, HEAD_DIM)
    return dict(
        hidden=draw_normal(part_keys[0], (SEQ_COUNT, MODEL_DIM), 1.0),
        positions=draw_positions(part_keys[1]),
        expert_ids=draw_routes(part_keys[2]),
        k_cache=draw_normal(part_keys[3], cache_shape, 1.0),
        v_cache=draw_normal(part_keys[4], cache_shape, 1.0),
        w_query=draw_normal(shared[0], (NUM_LAYERS, MODEL_DIM, Q_WIDTH), MODEL_DIM ** -0.5),
        w_key=draw_normal(shared[1], (NUM_LAYERS, MODEL_DIM, KV_WIDTH), MODEL_DIM ** -0.5),
        w_value=draw_normal(shared[2], (NUM_LAYERS, MODEL_DIM, KV_WIDTH), MODEL_DIM ** -0.5),
        w_out=draw_normal(shared[3], (NUM_LAYERS, Q_WIDTH, MODEL_DIM), 2.0 * Q_WIDTH ** -0.5),
        attn_gain=draw_gain(shared[4], (NUM_LAYERS, MODEL_DIM)),
        q_gain=draw_gain(shared[5], (NUM_LAYERS, Q_WIDTH)),
        k_gain=draw_gain(shared[6], (NUM_LAYERS, KV_WIDTH)),
        mlp_gain=draw_gain(shared[7], (NUM_LAYERS, MODEL_DIM)),
        w_router=draw_normal(shared[8], (MODEL_DIM, NUM_EXPERTS), MODEL_DIM ** -0.5),
        w_gate=draw_normal(shared[9], (NUM_EXPERTS, MODEL_DIM, FFN_DIM), MODEL_DIM ** -0.5),
        w_up=draw_normal(shared[10], (NUM_EXPERTS, MODEL_DIM, FFN_DIM), MODEL_DIM ** -0.5),
        w_down=draw_normal(shared[11], (NUM_EXPERTS, FFN_DIM, MODEL_DIM), NUM_EXPERTS * TOP_K ** -0.5 * FFN_DIM ** -0.5),
    )


def rms_norm(values, gain_vec):
    values = values.astype(jnp.float32)
    inv_rms = lax.rsqrt(jnp.mean(values * values, axis=-1, keepdims=True) + RMS_EPS)
    return values * inv_rms * gain_vec.astype(jnp.float32)


def rope_rotate(values, positions):
    half_dim = values.shape[-1] // 2
    frequencies = ROPE_BASE ** (-jnp.arange(half_dim, dtype=jnp.float32) / half_dim)
    angles = positions.astype(jnp.float32)[:, None] * frequencies[None, :]
    angles = angles.reshape((angles.shape[0],) + (1,) * (values.ndim - 2) + (half_dim,))
    cosines = jnp.cos(angles)
    sines = jnp.sin(angles)
    first_half = values[..., :half_dim]
    second_half = values[..., half_dim:]
    return jnp.concatenate([first_half * cosines - second_half * sines, second_half * cosines + first_half * sines], axis=-1)


def attention_layer(hidden, positions, k_layer, v_layer, w_query, w_key, w_value, w_out, attn_gain, q_gain, k_gain):
    head_group = NUM_HEADS // KV_HEADS
    normed = rms_norm(hidden, attn_gain).astype(jnp.bfloat16)
    q_heads = rms_norm(jnp.dot(normed, w_query, preferred_element_type=jnp.float32), q_gain)
    key_row = rms_norm(jnp.dot(normed, w_key, preferred_element_type=jnp.float32), k_gain)
    value_row = jnp.dot(normed, w_value, preferred_element_type=jnp.float32).astype(jnp.bfloat16)
    value_row = value_row.reshape(SEQ_COUNT, KV_HEADS, HEAD_DIM)
    q_heads = rope_rotate(q_heads.reshape(SEQ_COUNT, KV_HEADS, head_group, HEAD_DIM), positions).astype(jnp.bfloat16)
    key_row = rope_rotate(key_row.reshape(SEQ_COUNT, KV_HEADS, HEAD_DIM), positions).astype(jnp.bfloat16)
    hit_mask = (jnp.arange(CACHE_LEN)[None, :] == positions[:, None])[:, :, None, None]
    k_layer = jnp.where(hit_mask, key_row[:, None], k_layer)
    v_layer = jnp.where(hit_mask, value_row[:, None], v_layer)
    scores = jnp.einsum('bkgd,bskd->bkgs', q_heads.astype(jnp.float32), k_layer.astype(jnp.float32)) * HEAD_DIM ** -0.5
    valid_mask = (jnp.arange(CACHE_LEN)[None, :] <= positions[:, None])[:, None, None, :]
    scores = jnp.where(valid_mask, scores, -1e30)
    prob_vals = jax.nn.softmax(scores, axis=-1).astype(jnp.bfloat16)
    mixed_out = jnp.einsum('bkgs,bskd->bkgd', prob_vals.astype(jnp.float32), v_layer.astype(jnp.float32))
    mixed_out = mixed_out.astype(jnp.bfloat16).reshape(SEQ_COUNT, Q_WIDTH)
    hidden = (hidden.astype(jnp.float32) + jnp.dot(mixed_out, w_out, preferred_element_type=jnp.float32)).astype(jnp.bfloat16)
    return hidden, k_layer, v_layer


def moe_layer(hidden, routes, mlp_gain, w_router, w_gate, w_up, w_down):
    normed = rms_norm(hidden, mlp_gain).astype(jnp.bfloat16)
    router_prob = jax.nn.softmax(jnp.dot(normed, w_router, preferred_element_type=jnp.float32), axis=-1)
    gate_vals = jnp.take_along_axis(router_prob, routes, axis=1)
    flat_ids = routes.reshape(-1)
    sort_order = jnp.argsort(flat_ids, stable=True)
    counts = jnp.sum(flat_ids[:, None] == jnp.arange(NUM_EXPERTS)[None, :], axis=0, dtype=jnp.int32)
    starts = jnp.cumsum(counts) - counts
    per_expert = EP_GROUPS * CAPACITY
    padded = jnp.concatenate([sort_order, jnp.zeros((per_expert,), sort_order.dtype)])

    def expert_rows(item_pair):
        expert, start_at = item_pair
        copies = lax.dynamic_slice(padded, (start_at,), (per_expert,))
        token_rows = normed[copies // TOP_K]
        gate_act = jnp.dot(token_rows, w_gate[expert], preferred_element_type=jnp.float32)
        up_act = jnp.dot(token_rows, w_up[expert], preferred_element_type=jnp.float32)
        hidden_act = (jax.nn.silu(gate_act) * up_act).astype(jnp.bfloat16)
        return jnp.dot(hidden_act, w_down[expert], preferred_element_type=jnp.float32).astype(jnp.bfloat16)

    outputs = lax.map(expert_rows, (jnp.arange(NUM_EXPERTS), starts))
    copy_rank = jnp.argsort(sort_order, stable=True)
    within = copy_rank - starts[flat_ids]
    picked = outputs[flat_ids, within].reshape(SEQ_COUNT, TOP_K, MODEL_DIM)
    moe_out = jnp.sum(gate_vals[:, :, None] * picked.astype(jnp.float32), axis=1)
    return (hidden.astype(jnp.float32) + moe_out).astype(jnp.bfloat16)


def reference(hidden, positions, expert_ids, k_cache, v_cache, w_query, w_key, w_value, w_out, attn_gain, q_gain, k_gain, mlp_gain, w_router, w_gate, w_up, w_down):
    k_layers = []
    v_layers = []
    for layer_idx in range(NUM_LAYERS):
        hidden, k_layer, v_layer = attention_layer(hidden, positions, k_cache[layer_idx], v_cache[layer_idx], w_query[layer_idx], w_key[layer_idx], w_value[layer_idx], w_out[layer_idx], attn_gain[layer_idx], q_gain[layer_idx], k_gain[layer_idx])
        k_layers.append(k_layer)
        v_layers.append(v_layer)
        hidden = moe_layer(hidden, expert_ids[layer_idx], mlp_gain[layer_idx], w_router, w_gate, w_up, w_down)
    return hidden, jnp.stack(k_layers), jnp.stack(v_layers)
```

```python
import functools

import jax
import jax.numpy as jnp
from jax import lax
from jax.experimental import pallas as pl
from jax.experimental.pallas import tpu as pltpu
from jax.sharding import PartitionSpec as P

RMS_EPS = 1e-5
ROPE_BASE = 10000.0
CAP = 16
SLOTS = 5
F32 = jnp.float32
BF16 = jnp.bfloat16
ANY = pl.BlockSpec(memory_space=pl.ANY)
VMEM = pl.BlockSpec(memory_space=pltpu.VMEM)
SMEM = pl.BlockSpec(memory_space=pltpu.SMEM)
MESH = pl.DeviceIdType.MESH
NT = (((1,), (1,)), ((), ()))


def rms_rows(values, gain_row):
    inv_rms = lax.rsqrt(jnp.mean(values * values, axis=-1, keepdims=True) + RMS_EPS)
    return values * inv_rms * gain_row


def attn_kernel(layer, pos_ref, x_ref, cos_ref, sin_ref, attn_gain, q_gain, k_gain, mlp_gain, router_ref, member_ref,
                wq, wk, wv, wo, k_in, v_in, *rest):
    if layer > 0:
        rest = rest[2:]
    (x1_ref, h2_ref, gt_ref, k_out, v_out,
     wbuf, kbuf, vbuf, h_buf, lin, q2d, k2d, v2d, o2d, mixed, wsem, csem, osem) = rest
    rows, dim = x_ref.shape
    heads, hd = k_in.shape[3], k_in.shape[4]
    cache_len = k_in.shape[2]
    half = dim // 2

    def wcopy(i):
        src = (wq, wk, wv, wo)[i // 2]
        return pltpu.make_async_copy(src.at[layer, :, pl.ds((i % 2) * half, half)], wbuf.at[i], wsem.at[i])

    kcopy = pltpu.make_async_copy(k_in.at[layer], kbuf, csem.at[0])
    vcopy = pltpu.make_async_copy(v_in.at[layer], vbuf, csem.at[1])
    for i in range(4):
        wcopy(i).start()
    kcopy.start()
    for i in range(4, 6):
        wcopy(i).start()
    vcopy.start()
    for i in range(6, 8):
        wcopy(i).start()

    x = x_ref[...].astype(F32)
    h_buf[...] = rms_rows(x, attn_gain[layer:layer + 1, :]).astype(BF16)
    cos = cos_ref[...]
    sin = sin_ref[...]

    def project(which):
        for j in range(2):
            wcopy(2 * which + j).wait()
            lin[:, j * half:(j + 1) * half] = jnp.dot(h_buf[...], wbuf[2 * which + j], preferred_element_type=F32)

    def spread(gain_ref, dst):
        values = lin[...]
        inv_rms = lax.rsqrt(jnp.mean(values * values, axis=-1, keepdims=True) + RMS_EPS)
        for h in range(heads):
            cols = slice(h * hd, (h + 1) * hd)
            part = lin[:, cols] * inv_rms * gain_ref[layer:layer + 1, cols]
            part = part * cos + pltpu.roll(part, hd // 2, 1) * sin
            dst[pl.ds(h, rows, stride=heads), :] = part

    project(0)
    spread(q_gain, q2d)
    project(1)
    spread(k_gain, k2d)
    project(2)
    for h in range(heads):
        v2d[pl.ds(h, rows, stride=heads), :] = lin[:, h * hd:(h + 1) * hd]
    kcopy.wait()
    vcopy.wait()

    span = cache_len * heads
    col = lax.broadcasted_iota(jnp.int32, (heads, span), 1)
    row = lax.broadcasted_iota(jnp.int32, (heads, span), 0)
    same_head = (col % heads) == row
    cache_row = jnp.where(same_head, col // heads, cache_len)
    scale = hd ** -0.5
    group = 8

    def out_copies(g):
        at = pl.ds(pl.multiple_of(g * group, group), group)
        return (pltpu.make_async_copy(kbuf.at[at], k_out.at[layer, at], osem.at[0, g]),
                pltpu.make_async_copy(vbuf.at[at], v_out.at[layer, at], osem.at[1, g]))

    def attend(g, carry):
        outs = []
        for i in range(group):
            b = g * group + i
            p = pos_ref[b]
            at = pl.ds(pl.multiple_of(b * heads, heads), heads)
            kbuf[b, p] = k2d[at, :].astype(BF16)
            vbuf[b, p] = v2d[at, :].astype(BF16)
            kmat = kbuf[b].reshape(span, hd)
            scores = lax.dot_general(q2d[at, :].astype(BF16), kmat, NT, preferred_element_type=F32) * scale
            valid = cache_row <= p
            scores = jnp.where(valid, scores, -1e30)
            peak = jnp.max(scores, axis=-1, keepdims=True)
            weight = jnp.where(valid, jnp.exp(scores - peak), 0.0)
            outs.append((weight / jnp.sum(weight, axis=-1, keepdims=True)).astype(BF16))
        for i in range(group):
            b = g * group + i
            at = pl.ds(pl.multiple_of(b * heads, heads), heads)
            o2d[at, :] = jnp.dot(outs[i], vbuf[b].reshape(span, hd), preferred_element_type=F32)

        @pl.when(g > 0)
        def _():
            for copy in out_copies(g - 1):
                copy.start()
        return carry

    groups = rows // group
    lax.fori_loop(0, groups, attend, 0)
    for h in range(heads):
        mixed[:, h * hd:(h + 1) * hd] = o2d[pl.ds(h, rows, stride=heads), :].astype(BF16)
    for copy in out_copies(groups - 1):
        copy.start()
    for j in range(2):
        cols = slice(j * half, (j + 1) * half)
        wcopy(6 + j).wait()
        lin[:, cols] = x_ref[:, cols].astype(F32) + jnp.dot(mixed[...], wbuf[6 + j], preferred_element_type=F32)
    x1 = lin[...].astype(BF16)
    x1_ref[...] = x1
    h2 = rms_rows(x1.astype(F32), mlp_gain[layer:layer + 1, :]).astype(BF16)
    h2_ref[...] = h2
    logits = lax.dot_general(router_ref[...], jnp.concatenate([h2, h2], axis=0), NT, preferred_element_type=F32)
    logits = jnp.exp(logits - jnp.max(logits, axis=0, keepdims=True))
    probs = logits / jnp.sum(logits, axis=0, keepdims=True)
    gt_ref[...] = jnp.where(member_ref[layer] > 0.5, probs, -1.0)
    for g in range(groups):
        for copy in out_copies(g):
            copy.wait()


def attention(layer, pos, x, cos, sin, attn_gain, q_gain, k_gain, mlp_gain, router_t, member, wq, wk, wv, wo, k_in, v_in, prev):
    rows, dim = x.shape
    _, _, cache_len, heads, hd = k_in.shape
    aliases = {} if prev is None else {16: 3, 17: 4}
    prev = () if prev is None else prev
    groups = rows // 8
    return pl.pallas_call(
        functools.partial(attn_kernel, layer),
        name="attn",
        out_shape=(
            jax.ShapeDtypeStruct((rows, dim), BF16),
            jax.ShapeDtypeStruct((rows, dim), BF16),
            jax.ShapeDtypeStruct(member.shape[1:], F32),
            jax.ShapeDtypeStruct(k_in.shape, BF16),
            jax.ShapeDtypeStruct(v_in.shape, BF16),
        ),
        in_specs=[SMEM] + [VMEM] * 9 + [ANY] * (6 + len(prev)),
        out_specs=(VMEM, VMEM, VMEM, ANY, ANY),
        scratch_shapes=[
            pltpu.VMEM((8, dim, dim // 2), BF16),
            pltpu.VMEM(k_in.shape[1:], BF16),
            pltpu.VMEM(v_in.shape[1:], BF16),
            pltpu.VMEM((rows, dim), BF16),
            pltpu.VMEM((rows, dim), F32),
            pltpu.VMEM((rows * heads, hd), F32),
            pltpu.VMEM((rows * heads, hd), F32),
            pltpu.VMEM((rows * heads, hd), F32),
            pltpu.VMEM((rows * heads, hd), F32),
            pltpu.VMEM((rows, dim), BF16),
            pltpu.SemaphoreType.DMA((8,)),
            pltpu.SemaphoreType.DMA((2,)),
            pltpu.SemaphoreType.DMA((2, groups)),
        ],
        input_output_aliases=aliases,
        compiler_params=pltpu.CompilerParams(vmem_limit_bytes=60 * 2 ** 20),
    )(pos, x, cos, sin, attn_gain, q_gain, k_gain, mlp_gain, router_t, member, wq, wk, wv, wo, k_in, v_in, *prev)


def moe_kernel(h2_ref, gt_ref, x1_ref, wg, wu, wd, out_ref,
               ring, xall, xe, act, ybuf, pick, chi, cmid, clo, part, dr, sbuf, rr, gtall,
               wsem, a_send, a_recv, d_send, d_recv, g_send, g_recv, p_send, p_recv, r_send, r_recv):
    rows, dim = h2_ref.shape
    experts, _, ffn = wg.shape
    slots = pick.shape[0] // experts
    tokens = xall.shape[0]
    blocks = out_ref.shape[1] // ybuf.shape[1]
    bcols = ybuf.shape[1]
    pairs = experts + blocks
    half_rows = ring.shape[2] // 2

    def start_experts(i, slot):
        pltpu.make_async_copy(wg.at[i], ring.at[slot, 0], wsem.at[slot, 0]).start()
        pltpu.make_async_copy(wu.at[i], ring.at[slot, 1], wsem.at[slot, 1]).start()

    def start_down(c, slot):
        cols = pl.ds(pl.multiple_of(c * bcols, bcols), bcols)
        for e in range(experts):
            part_of, quarter = e // 4, e % 4
            pltpu.make_async_copy(
                wd.at[e, :, cols],
                ring.at[slot, part_of, pl.ds((quarter // 2) * half_rows, half_rows), pl.ds((quarter % 2) * bcols, bcols)],
                wsem.at[slot, part_of]).start()

    def wait_weights(slot, part_of):
        pltpu.make_async_copy(wg.at[0], ring.at[slot, part_of], wsem.at[slot, part_of]).wait()

    for i in range(SLOTS):
        start_experts(i, i)

    me = lax.axis_index("ep")
    core = lax.rem(me, 2)
    chip = lax.div(me, 2)
    at_x = lax.rem(chip, 2)
    at_y = lax.div(chip, 2)

    def chip_at(r):
        cx = 1 - at_x if r % 2 else at_x
        cy = 1 - at_y if r // 2 else at_y
        return 2 * cy + cx

    def device_at(q):
        return 2 * chip_at(q // 2) + (1 - core if q % 2 else core)

    barrier = pltpu.get_barrier_semaphore()
    for q in range(1, 8):
        pl.semaphore_signal(barrier, inc=1, device_id={"ep": device_at(q)}, device_id_type=MESH)
    pl.semaphore_wait(barrier, 7)

    def rows_of(dev):
        return pl.ds(pl.multiple_of(dev * rows, rows), rows)

    def experts_of(dev):
        return pl.ds(pl.multiple_of(dev * experts, experts), experts)

    def remote(src, dst, send, recv, dev):
        return pltpu.make_async_remote_copy(src_ref=src, dst_ref=dst, send_sem=send, recv_sem=recv,
                                            device_id={"ep": dev}, device_id_type=MESH)

    partner = device_at(1)
    gates = [remote(gt_ref.at[experts_of(device_at(q))], gtall.at[me], g_send.at[q], g_recv.at[q], device_at(q))
             for q in range(1, 8)]
    across = [remote(h2_ref, xall.at[rows_of(me)], a_send.at[r], a_recv.at[r], device_at(2 * r)) for r in range(1, 4)]
    own = remote(h2_ref, xall.at[rows_of(me)], d_send.at[0], d_recv.at[0], partner)
    for copy in gates:
        copy.start()
    for copy in across:
        copy.start()
    own.start()
    xall[rows_of(me), :] = h2_ref[...]
    gtall[me] = gt_ref[experts_of(me), :]
    for copy in gates:
        copy.wait_recv()

    lane = lax.broadcasted_iota(jnp.int32, (experts, 2 * rows), 1)
    gate_rows = jnp.concatenate(
        [jnp.where(lane < rows, gtall[2 * j], gtall[2 * j + 1]) for j in range(tokens // (2 * rows))], axis=1)
    chosen = gate_rows >= 0.0
    upper = (lax.broadcasted_iota(jnp.int32, (tokens, tokens), 0)
             <= lax.broadcasted_iota(jnp.int32, (tokens, tokens), 1))
    counted = jnp.dot(jnp.where(chosen, 1.0, 0.0).astype(BF16), jnp.where(upper, 1.0, 0.0).astype(BF16),
                      preferred_element_type=F32)
    ranks = jnp.where(chosen, counted - 1.0, -1.0)
    slot_of = lax.broadcasted_iota(jnp.int32, (slots, tokens), 0).astype(F32)
    for e in range(experts):
        pick[e * slots:(e + 1) * slots, :] = jnp.where(slot_of == ranks[e:e + 1, :], 1.0, 0.0).astype(BF16)
    stacked = jnp.concatenate([gate_rows, ranks, jnp.zeros((128 - 2 * experts, tokens), F32)], axis=0)
    columns = jnp.transpose(stacked)
    slot_at = lax.broadcasted_iota(jnp.int32, (tokens, slots), 1).astype(F32)
    for e in range(experts):
        gated = jnp.where(slot_at == columns[:, experts + e:experts + e + 1], columns[:, e:e + 1], 0.0)
        at = slice(e * slots, (e + 1) * slots)
        high = gated.astype(BF16)
        rest = gated - high.astype(F32)
        middle = rest.astype(BF16)
        chi[:, at] = high
        cmid[:, at] = middle
        clo[:, at] = (rest - middle.astype(F32)).astype(BF16)

    passed = []
    for r in range(1, 4):
        across[r - 1].wait_recv()
        block = xall.at[rows_of(device_at(2 * r))]
        copy = remote(block, block, d_send.at[r], d_recv.at[r], partner)
        copy.start()
        passed.append(copy)
    own.wait_recv()
    for copy in passed:
        copy.wait_recv()

    def expert_step(e, carry):
        slot = lax.rem(e, SLOTS)
        at = pl.ds(pl.multiple_of(e * slots, slots), slots)
        xe[...] = jnp.dot(pick[at, :], xall[...], preferred_element_type=F32).astype(BF16)
        wait_weights(slot, 0)
        gate_act = jnp.dot(xe[...], ring[slot, 0], preferred_element_type=F32)
        wait_weights(slot, 1)
        up_act = jnp.dot(xe[...], ring[slot, 1], preferred_element_type=F32)
        act[at, :] = (jax.nn.silu(gate_act) * up_act).astype(BF16)

        @pl.when(e + SLOTS < experts)
        def _():
            start_experts(e + SLOTS, slot)

        @pl.when(jnp.logical_and(e + SLOTS >= experts, e + SLOTS < pairs))
        def _():
            start_down(e + SLOTS - experts, slot)
        return carry

    lax.fori_loop(0, experts, expert_step, 0)

    def pair_copy(c):
        return remote(part.at[lax.rem(c, 2), :, 1 - core], dr.at[c], p_send.at[c], p_recv.at[c], partner)

    def chip_copy(c, r):
        return remote(sbuf.at[c, chip_at(r)], rr.at[c, r - 1], r_send.at[c, r - 1], r_recv.at[c, r - 1], device_at(2 * r))

    def relay(c):
        copy = pair_copy(c)
        copy.wait_send()
        copy.wait_recv()
        sbuf[c] = part[lax.rem(c, 2), :, core] + dr[c]
        for r in range(1, 4):
            chip_copy(c, r).start()

    def block_step(c, carry):
        slot = lax.rem(experts + c, SLOTS)
        for e in range(experts):
            part_of, quarter = e // 4, e % 4
            if quarter == 0:
                wait_weights(slot, part_of)
            down = ring[slot, part_of, (quarter // 2) * half_rows:(quarter // 2 + 1) * half_rows,
                        (quarter % 2) * bcols:(quarter % 2 + 1) * bcols]
            ybuf[e * slots:(e + 1) * slots, :] = jnp.dot(
                act[e * slots:(e + 1) * slots, :], down, preferred_element_type=F32).astype(BF16)

        @pl.when(c > 0)
        def _():
            relay(c - 1)

        def combine(m, inner):
            at = pl.ds(pl.multiple_of(m * 2 * rows, 2 * rows), 2 * rows)
            total = jnp.dot(chi[at, :], ybuf[...], preferred_element_type=F32)
            total += jnp.dot(cmid[at, :], ybuf[...], preferred_element_type=F32)
            total += jnp.dot(clo[at, :], ybuf[...], preferred_element_type=F32)
            part[lax.rem(c, 2), m] = total.reshape(2, rows, bcols)
            return inner

        lax.fori_loop(0, tokens // (2 * rows), combine, 0)
        pair_copy(c).start()
        return carry

    lax.fori_loop(0, blocks, block_step, 0)
    relay(blocks - 1)
    for c in range(blocks):
        for r in range(1, 4):
            chip_copy(c, r).wait_recv()
        cols = slice(c * bcols, (c + 1) * bcols)
        total = sbuf[c, chip] + rr[c, 0] + rr[c, 1] + rr[c, 2]
        out_ref[:, cols] = (x1_ref[:, cols].astype(F32) + total).astype(BF16)
    for copy in gates + across + [own] + passed:
        copy.wait_send()
    for c in range(blocks):
        for r in range(1, 4):
            chip_copy(c, r).wait_send()


def moe(h2, gt, x1, wg, wu, wd, groups):
    rows, dim = h2.shape
    experts, _, ffn = wg.shape
    tokens = rows * groups
    slots = CAP * groups
    blocks = 4
    bcols = dim // blocks
    chips = groups // 2
    dma = pltpu.SemaphoreType.DMA
    return pl.pallas_call(
        moe_kernel,
        name="moe",
        out_shape=jax.ShapeDtypeStruct((rows, dim), BF16),
        in_specs=[VMEM] * 3 + [ANY] * 3,
        out_specs=VMEM,
        scratch_shapes=[
            pltpu.VMEM((SLOTS, 2, dim, ffn), BF16),
            pltpu.VMEM((tokens, dim), BF16),
            pltpu.VMEM((slots, dim), BF16),
            pltpu.VMEM((experts * slots, ffn), BF16),
            pltpu.VMEM((experts * slots, bcols), BF16),
            pltpu.VMEM((experts * slots, tokens), BF16),
            pltpu.VMEM((tokens, experts * slots), BF16),
            pltpu.VMEM((tokens, experts * slots), BF16),
            pltpu.VMEM((tokens, experts * slots), BF16),
            pltpu.VMEM((2, chips, 2, rows, bcols), F32),
            pltpu.VMEM((blocks, chips, rows, bcols), F32),
            pltpu.VMEM((blocks, chips, rows, bcols), F32),
            pltpu.VMEM((blocks, chips - 1, rows, bcols), F32),
            pltpu.VMEM((groups, experts, 2 * rows), F32),
            dma((SLOTS, 2)),
            dma((4,)), dma((4,)), dma((4,)), dma((4,)), dma((8,)), dma((8,)),
            dma((blocks,)), dma((blocks,)), dma((blocks, chips - 1)), dma((blocks, chips - 1)),
        ],
        compiler_params=pltpu.CompilerParams(collective_id=0, has_side_effects=True, vmem_limit_bytes=62 * 2 ** 20),
    )(h2, gt, x1, wg, wu, wd)


def solution(mesh):
    groups = mesh.shape['ep']
    batch_axes = ('dp', 'ep')

    def device_step(hidden, positions, expert_ids, k_cache, v_cache, w_query, w_key, w_value, w_out, attn_gain, q_gain, k_gain, mlp_gain, w_router, w_gate, w_up, w_down):
        hd = k_cache.shape[-1]
        half_dim = hd // 2
        frequencies = ROPE_BASE ** (-jnp.arange(half_dim, dtype=F32) / half_dim)
        angles = positions.astype(F32)[:, None] * frequencies[None, :]
        cosines = jnp.cos(angles)
        sines = jnp.sin(angles)
        cos = jnp.concatenate([cosines, cosines], axis=-1)
        sin = jnp.concatenate([-sines, sines], axis=-1)
        num_experts = w_router.shape[1]
        hits = expert_ids[:, None, :, :] == jnp.arange(num_experts, dtype=jnp.int32)[None, :, None, None]
        member = jnp.any(hits, axis=-1).astype(F32)
        member = jnp.concatenate([member, member], axis=-1)
        router_t = w_router.T
        caches = None
        for layer in range(expert_ids.shape[0]):
            x1, h2, gt, k_new, v_new = attention(layer, positions, hidden, cos, sin, attn_gain, q_gain, k_gain, mlp_gain, router_t, member,
                                                 w_query, w_key, w_value, w_out, k_cache, v_cache, caches)
            caches = (k_new, v_new)
            hidden = moe(h2, gt, x1, w_gate, w_up, w_down, groups)
        return hidden, caches[0], caches[1]

    row_spec = P(batch_axes, None)
    cache_spec = P(None, batch_axes, None, None, None)
    full_spec = P()
    expert_spec = P('ep', None, None)
    in_specs = (row_spec, P(batch_axes), P(None, batch_axes, None), cache_spec, cache_spec, full_spec, full_spec, full_spec, full_spec, full_spec, full_spec, full_spec, full_spec, full_spec, expert_spec, expert_spec, expert_spec)
    return jax.shard_map(device_step, mesh=mesh, in_specs=in_specs, out_specs=(row_spec, cache_spec, cache_spec), check_vma=False)
```

```python
import functools
import math

import jax
import jax.numpy as jnp
from jax import lax
from jax.experimental import pallas as pl
from jax.experimental.pallas import tpu as pltpu
from jax.sharding import PartitionSpec as P

RMS_EPS = 1e-5
ROPE_BASE = 10000.0
CAP = 16
SLOTS = 5
FCOLS = 512
F32 = jnp.float32
BF16 = jnp.bfloat16
ANY = pl.BlockSpec(memory_space=pl.ANY)
VMEM = pl.BlockSpec(memory_space=pltpu.VMEM)
SMEM = pl.BlockSpec(memory_space=pltpu.SMEM)
MESH = pl.DeviceIdType.MESH
NT = (((1,), (1,)), ((), ()))


def rms_rows(values, gain_row):
    inv_rms = lax.rsqrt(jnp.mean(values * values, axis=-1, keepdims=True) + RMS_EPS)
    return values * inv_rms * gain_row


def attn_kernel(layer, pos_ref, x_hbm, ids_hbm, attn_gain_hbm, q_gain_hbm, k_gain_hbm, mlp_gain_hbm, router_hbm,
                wq, wk, wv, wo, k_in, v_in, *rest):
    if layer > 0:
        rest = rest[2:]
    (x1_ref, h2_ref, gt_ref, k_out, v_out,
     x_ref, ids_ref, attn_gain, q_gain, k_gain, mlp_gain, router_ref, angle,
     wbuf, kbuf, vbuf, h_buf, lin, q2d, k2d, probs, mixed, ssem, wsem, csem, osem) = rest
    rows, dim = x_ref.shape
    heads, hd = k_in.shape[3], k_in.shape[4]
    cache_len = k_in.shape[2]
    half = dim // 2
    experts = router_ref.shape[0]

    def wcopy(i):
        src = (wq, wk, wv, wo)[i // 2]
        return pltpu.make_async_copy(src.at[layer, :, pl.ds((i % 2) * half, half)], wbuf.at[i], wsem.at[i])

    kcopy = pltpu.make_async_copy(k_in.at[layer], kbuf, csem.at[0])
    vcopy = pltpu.make_async_copy(v_in.at[layer], vbuf, csem.at[1])
    small = [pltpu.make_async_copy(src, dst, ssem.at[n]) for n, (src, dst) in enumerate((
        (x_hbm, x_ref), (attn_gain_hbm, attn_gain), (ids_hbm, ids_ref), (q_gain_hbm, q_gain), (k_gain_hbm, k_gain),
        (mlp_gain_hbm, mlp_gain), (router_hbm, router_ref)))]
    for copy in small:
        copy.start()
    for i in range(4):
        wcopy(i).start(priority=1)
    after = {0: [kcopy], 1: [wcopy(4)], 2: [wcopy(5)], 3: [vcopy], 4: [wcopy(6)], 5: [wcopy(7)]}
    for copy in small:
        copy.wait()
    x = x_ref[...].astype(F32)
    h_buf[...] = rms_rows(x, attn_gain[layer:layer + 1, :]).astype(BF16)
    lane = lax.broadcasted_iota(jnp.int32, (1, hd), 1)
    exponent = (lane % (hd // 2)).astype(F32) / (hd // 2)
    frequencies = jnp.exp(exponent * -math.log(ROPE_BASE))
    for b in range(rows):
        angle[b:b + 1, :] = frequencies * pos_ref[b].astype(F32)
    angles = angle[...]
    cos = jnp.cos(angles)
    sin = jnp.where(lane < hd // 2, -1.0, 1.0) * jnp.sin(angles)
    expert_row = lax.broadcasted_iota(jnp.int32, (experts, 128), 0)
    wide_ids = jnp.concatenate([ids_ref[layer]] * (128 // rows), axis=1)
    hits = expert_row == wide_ids[0:1, :]
    for j in range(1, wide_ids.shape[0]):
        hits = jnp.logical_or(hits, expert_row == wide_ids[j:j + 1, :])
    member = jnp.where(hits, 1.0, 0.0)

    def project(which):
        for j in range(2):
            wcopy(2 * which + j).wait()
            for copy in after.get(2 * which + j, ()):
                copy.start(priority=1)
            lin[:, j * half:(j + 1) * half] = jnp.dot(h_buf[...], wbuf[2 * which + j], preferred_element_type=F32)

    def spread(gain_ref, dst):
        values = lin[...]
        inv_rms = lax.rsqrt(jnp.mean(values * values, axis=-1, keepdims=True) + RMS_EPS)
        for h in range(heads):
            cols = slice(h * hd, (h + 1) * hd)
            part = lin[:, cols] * inv_rms * gain_ref[layer:layer + 1, cols]
            part = part * cos + pltpu.roll(part, hd // 2, 1) * sin
            dst[pl.ds(h, rows, stride=heads), :] = part

    project(0)
    spread(q_gain, q2d)
    project(1)
    spread(k_gain, k2d)
    kcopy.wait()

    span = cache_len * heads
    col = lax.broadcasted_iota(jnp.int32, (heads, span), 1)
    row = lax.broadcasted_iota(jnp.int32, (heads, span), 0)
    same_head = (col % heads) == row
    cache_row = jnp.where(same_head, col // heads, cache_len)
    scale = hd ** -0.5
    group = 8
    groups = rows // group

    def out_copy(which, g):
        at = pl.ds(pl.multiple_of(g * group, group), group)
        src, dst = ((kbuf, k_out), (vbuf, v_out))[which]
        return pltpu.make_async_copy(src.at[at], dst.at[layer, at], osem.at[which, g])

    def heads_of(b):
        return pl.ds(pl.multiple_of(b * heads, heads), heads)

    def score(g, carry):
        for i in range(group):
            b = g * group + i
            p = pos_ref[b]
            kbuf[b, p] = k2d[heads_of(b), :].astype(BF16)
            kmat = kbuf[b].reshape(span, hd)
            scores = lax.dot_general(q2d[heads_of(b), :].astype(BF16), kmat, NT, preferred_element_type=F32) * scale
            valid = cache_row <= p
            scores = jnp.where(valid, scores, -1e30)
            peak = jnp.max(scores, axis=-1, keepdims=True)
            weight = jnp.where(valid, jnp.exp(scores - peak), 0.0)
            probs[heads_of(b), :] = (weight / jnp.sum(weight, axis=-1, keepdims=True)).astype(BF16)

        @pl.when(g > 0)
        def _():
            out_copy(0, g - 1).start()
        return carry

    lax.fori_loop(0, groups, score, 0)
    project(2)
    out_copy(0, groups - 1).start()
    v2d = q2d
    o2d = k2d
    for h in range(heads):
        v2d[pl.ds(h, rows, stride=heads), :] = lin[:, h * hd:(h + 1) * hd]
    vcopy.wait()

    def mix(g, carry):
        for i in range(group):
            b = g * group + i
            vbuf[b, pos_ref[b]] = v2d[heads_of(b), :].astype(BF16)
            o2d[heads_of(b), :] = jnp.dot(probs[heads_of(b), :], vbuf[b].reshape(span, hd), preferred_element_type=F32)

        @pl.when(g > 0)
        def _():
            out_copy(1, g - 1).start()
        return carry

    lax.fori_loop(0, groups, mix, 0)
    for h in range(heads):
        mixed[:, h * hd:(h + 1) * hd] = o2d[pl.ds(h, rows, stride=heads), :].astype(BF16)
    out_copy(1, groups - 1).start()
    for j in range(2):
        cols = slice(j * half, (j + 1) * half)
        wcopy(6 + j).wait()
        lin[:, cols] = x_ref[:, cols].astype(F32) + jnp.dot(mixed[...], wbuf[6 + j], preferred_element_type=F32)
    x1 = lin[...].astype(BF16)
    x1_ref[...] = x1
    h2 = rms_rows(x1.astype(F32), mlp_gain[layer:layer + 1, :]).astype(BF16)
    h2_ref[...] = h2
    logits = lax.dot_general(router_ref[...], jnp.concatenate([h2] * (128 // rows), axis=0), NT, preferred_element_type=F32)
    logits = jnp.exp(logits - jnp.max(logits, axis=0, keepdims=True))
    router_probs = logits / jnp.sum(logits, axis=0, keepdims=True)
    gt_ref[...] = jnp.where(member > 0.5, router_probs, -1.0)
    for g in range(groups):
        for which in range(2):
            out_copy(which, g).wait()


def attention(layer, pos, x, ids, attn_gain, q_gain, k_gain, mlp_gain, router_t, wq, wk, wv, wo, k_in, v_in, prev):
    rows, dim = x.shape
    _, _, cache_len, heads, hd = k_in.shape
    aliases = {} if prev is None else {14: 3, 15: 4}
    prev = () if prev is None else prev
    groups = rows // 8
    return pl.pallas_call(
        functools.partial(attn_kernel, layer),
        name="attn",
        out_shape=(
            jax.ShapeDtypeStruct((rows, dim), BF16),
            jax.ShapeDtypeStruct((rows, dim), BF16),
            jax.ShapeDtypeStruct((router_t.shape[0], 128), F32),
            jax.ShapeDtypeStruct(k_in.shape, BF16),
            jax.ShapeDtypeStruct(v_in.shape, BF16),
        ),
        in_specs=[SMEM] + [ANY] * (13 + len(prev)),
        out_specs=(VMEM, VMEM, VMEM, ANY, ANY),
        scratch_shapes=[
            *[pltpu.VMEM(a.shape, a.dtype) for a in (x, ids, attn_gain, q_gain, k_gain, mlp_gain, router_t)],
            pltpu.VMEM((rows, hd), F32),
            pltpu.VMEM((8, dim, dim // 2), BF16),
            pltpu.VMEM(k_in.shape[1:], BF16),
            pltpu.VMEM(v_in.shape[1:], BF16),
            pltpu.VMEM((rows, dim), BF16),
            pltpu.VMEM((rows, dim), F32),
            pltpu.VMEM((rows * heads, hd), F32),
            pltpu.VMEM((rows * heads, hd), F32),
            pltpu.VMEM((rows * heads, cache_len * heads), BF16),
            pltpu.VMEM((rows, dim), BF16),
            pltpu.SemaphoreType.DMA((7,)),
            pltpu.SemaphoreType.DMA((8,)),
            pltpu.SemaphoreType.DMA((2,)),
            pltpu.SemaphoreType.DMA((2, groups)),
        ],
        input_output_aliases=aliases,
        compiler_params=pltpu.CompilerParams(vmem_limit_bytes=60 * 2 ** 20),
    )(pos, x, ids, attn_gain, q_gain, k_gain, mlp_gain, router_t, wq, wk, wv, wo, k_in, v_in, *prev)


def moe_kernel(h2_hbm, gt_hbm, x1_hbm, wg, wu, wd, out_ref,
               h2_ref, gt_ref, x1_ref, ring, xall, xs, act, ybuf, pick, spread, terms, part, dr, sbuf, step1, step2, gtall,
               ssem, wsem, a_send, a_recv, f_send, f_recv, d_send, d_recv, g_send, g_recv, p_send, p_recv, u_send, u_recv, w_send, w_recv):
    rows, dim = h2_ref.shape
    experts, _, ffn = wg.shape
    groups = xs.shape[1] // CAP
    chips = groups // 2
    bcols = ybuf.shape[2]
    blocks = dim // bcols
    sub = bcols // 2
    pairs = experts + blocks
    half_rows = ring.shape[2] // 2
    hrows = rows // 2

    def start_experts(i, slot):
        pltpu.make_async_copy(wg.at[i], ring.at[slot, 0], wsem.at[slot, 0]).start(priority=1)
        pltpu.make_async_copy(wu.at[i], ring.at[slot, 1], wsem.at[slot, 1]).start(priority=1)

    def start_down(c, slot):
        cols = pl.ds(pl.multiple_of(c * bcols, bcols), bcols)
        for e in range(experts):
            part_of, quarter = e // 4, e % 4
            pltpu.make_async_copy(
                wd.at[e, :, cols],
                ring.at[slot, part_of, pl.ds((quarter // 2) * half_rows, half_rows), pl.ds((quarter % 2) * bcols, bcols)],
                wsem.at[slot, part_of]).start(priority=1)

    def wait_weights(slot, part_of):
        pltpu.make_async_copy(wg.at[0], ring.at[slot, part_of], wsem.at[slot, part_of]).wait()

    small = [pltpu.make_async_copy(src, dst, ssem.at[n]) for n, (src, dst) in enumerate((
        (h2_hbm, h2_ref), (gt_hbm, gt_ref), (x1_hbm, x1_ref)))]
    for copy in small:
        copy.start()
    for i in range(SLOTS):
        start_experts(i, i)

    me = lax.axis_index("ep")
    core = lax.rem(me, 2)
    chip = lax.div(me, 2)
    at_x = lax.rem(chip, 2)
    at_y = lax.div(chip, 2)

    def chip_at(r):
        cx = 1 - at_x if r % 2 else at_x
        cy = 1 - at_y if r // 2 else at_y
        return 2 * cy + cx

    def device_at(q):
        return 2 * chip_at(q // 2) + (1 - core if q % 2 else core)

    barrier = pltpu.get_barrier_semaphore()
    for q in range(1, 8):
        pl.semaphore_signal(barrier, inc=1, device_id={"ep": device_at(q)}, device_id_type=MESH)
    for copy in small:
        copy.wait()
    pl.semaphore_wait(barrier, 7)

    def rows_of(dev):
        return pl.ds(pl.multiple_of(dev * rows, rows), rows)

    def half_of(dev, k):
        return pl.ds(pl.multiple_of(dev * rows + k * hrows, hrows), hrows)

    def experts_of(dev):
        return pl.ds(pl.multiple_of(dev * experts, experts), experts)

    def remote(src, dst, send, recv, dev):
        return pltpu.make_async_remote_copy(src_ref=src, dst_ref=dst, send_sem=send, recv_sem=recv,
                                            device_id={"ep": dev}, device_id_type=MESH)

    partner = device_at(1)
    gates = [remote(gt_ref.at[experts_of(device_at(q))], gtall.at[me], g_send.at[q], g_recv.at[q], device_at(q))
             for q in range(1, 8)]

    def across(r, k):
        return remote(h2_ref.at[pl.ds(k * hrows, hrows)], xall.at[half_of(me, k)], a_send.at[r - 1, k], a_recv.at[r - 1, k],
                      device_at(2 * r))

    own = remote(h2_ref, xall.at[rows_of(me)], d_send.at[0, 0], d_recv.at[0, 0], partner)
    for copy in gates:
        copy.start()
    for r, k in ((1, 0), (2, 1), (1, 1), (2, 0)):
        across(r, k).start()
    own.start()
    xall[rows_of(me), :] = h2_ref[...]
    gtall[me] = gt_ref[experts_of(me), :]
    for copy in gates:
        copy.wait_recv()

    lane = lax.broadcasted_iota(jnp.int32, (experts, 2 * rows), 1)
    gate_rows = jnp.concatenate([jnp.where(lane < rows, gtall[2 * j], gtall[2 * j + 1]) for j in range(chips)], axis=0)
    chosen = gate_rows >= 0.0
    first = lax.broadcasted_iota(jnp.int32, (2 * rows, 2 * rows), 0)
    second = lax.broadcasted_iota(jnp.int32, (2 * rows, 2 * rows), 1)
    upper = jnp.logical_and(first <= second, first // rows == second // rows)
    counted = jnp.dot(jnp.where(chosen, 1.0, 0.0).astype(BF16), jnp.where(upper, 1.0, 0.0).astype(BF16),
                      preferred_element_type=F32)
    ranks = jnp.where(chosen, counted - 1.0, -1.0)
    slot_of = lax.broadcasted_iota(jnp.int32, (CAP, 2 * rows), 0).astype(F32)
    left = lax.broadcasted_iota(jnp.int32, (CAP, 2 * rows), 1) < rows
    width = experts * CAP
    for j in range(chips):
        for e in range(experts):
            line = slice(j * experts + e, j * experts + e + 1)
            hit = slot_of == ranks[line, :]
            at = slice(e * CAP, (e + 1) * CAP)
            pick[j, at, :] = jnp.where(jnp.logical_and(hit, left), 1.0, 0.0).astype(BF16)
            pick[j, width + e * CAP:width + (e + 1) * CAP, :] = jnp.where(
                jnp.logical_and(hit, jnp.logical_not(left)), 1.0, 0.0).astype(BF16)
            spread[j, at, :] = jnp.where(hit, gate_rows[line, :], 0.0)
    for j in range(chips):
        gated = jnp.transpose(spread[j])
        high = gated.astype(BF16)
        rest = gated - high.astype(F32)
        middle = rest.astype(BF16)
        low = (rest - middle.astype(F32)).astype(BF16)
        for k in range(2):
            for n, term in enumerate((high, middle, low)):
                terms[2 * j + k, n * rows:(n + 1) * rows, :] = term[k * rows:(k + 1) * rows, :]

    passed = [own]

    def hand_over(r, k):
        block = xall.at[half_of(device_at(2 * r), k)]
        copy = remote(block, block, d_send.at[r, k], d_recv.at[r, k], partner)
        copy.start()
        passed.append(copy)

    def forward(r, k):
        block = xall.at[half_of(device_at(2 * r), k)]
        return remote(block, block, f_send.at[k], f_recv.at[k], device_at(2 * (3 - r)))

    across(1, 0).wait_recv()
    ahead = [forward(1, 0)]
    ahead[0].start()
    hand_over(1, 0)
    across(2, 1).wait_recv()
    ahead.append(forward(2, 1))
    ahead[1].start()
    hand_over(2, 1)

    def take_rows(r):
        j = chip_at(r)
        chosen_rows = jnp.dot(pick[j], xall[pl.ds(pl.multiple_of(j * 2 * rows, 2 * rows), 2 * rows), :],
                              preferred_element_type=F32).astype(BF16)
        for k in range(2):
            for e in range(experts):
                xs[e, pl.ds(pl.multiple_of((2 * j + k) * CAP, CAP), CAP), :] = chosen_rows[k * width + e * CAP:k * width + (e + 1) * CAP, :]

    own.wait_recv()
    take_rows(0)
    across(1, 1).wait_recv()
    hand_over(1, 1)
    across(2, 0).wait_recv()
    hand_over(2, 0)
    passed[1].wait_recv()
    passed[3].wait_recv()
    take_rows(1)
    passed[2].wait_recv()
    passed[4].wait_recv()
    take_rows(2)
    for k in range(2):
        ahead[k].wait_recv()
        hand_over(3, k)
    passed[5].wait_recv()
    passed[6].wait_recv()
    take_rows(3)

    def expert_step(e, carry):
        slot = lax.rem(e, SLOTS)
        at = pl.ds(pl.multiple_of(e * groups * CAP, groups * CAP), groups * CAP)
        wait_weights(slot, 0)
        wait_weights(slot, 1)
        for n in range(ffn // FCOLS):
            cols = slice(n * FCOLS, (n + 1) * FCOLS)
            gate_act = jnp.dot(xs[e], ring[slot, 0, :, cols], preferred_element_type=F32)
            up_act = jnp.dot(xs[e], ring[slot, 1, :, cols], preferred_element_type=F32)
            act[at, cols] = (jax.nn.silu(gate_act) * up_act).astype(BF16)

        @pl.when(e + SLOTS < experts)
        def _():
            start_experts(e + SLOTS, slot)

        @pl.when(jnp.logical_and(e + SLOTS >= experts, e + SLOTS < pairs))
        def _():
            start_down(e + SLOTS - experts, slot)
        return carry

    lax.fori_loop(0, experts, expert_step, 0)

    def pair_copy(c):
        return remote(part.at[lax.rem(c, 2), :, 1 - core], dr.at[c], p_send.at[c], p_recv.at[c], partner)

    def first_copy(c, s, k):
        to = 1 + s
        return remote(sbuf.at[c, s, chip_at((to, 3)[k])], step1.at[c, s, k], u_send.at[c, s, k], u_recv.at[c, s, k],
                      device_at(2 * to))

    def second_copy(c, s):
        to = 2 - s
        return remote(sbuf.at[c, s, chip_at(to)], step2.at[c, s], w_send.at[c, s], w_recv.at[c, s], device_at(2 * to))

    def relay_pair(c):
        copy = pair_copy(c)
        copy.wait_send()
        copy.wait_recv()
        both = part[lax.rem(c, 2), :, core] + dr[c]
        for s in range(2):
            sbuf[c, s] = both[:, :, s * sub:(s + 1) * sub]
        for k in (1, 0):
            for s in range(2):
                first_copy(c, s, k).start()

    def relay_first(c):
        for s in range(2):
            first_copy(c, s, 1).wait_recv()
            to = chip_at(2 - s)
            sbuf[c, s, to] = sbuf[c, s, to] + step1[c, s, 1]
            second_copy(c, s).start()

    def finish(c):
        for s in range(2):
            first_copy(c, s, 0).wait_recv()
            second_copy(c, s).wait_recv()
            cols = pl.ds(pl.multiple_of(c * bcols + s * sub, sub), sub)
            total = sbuf[c, s, chip] + step1[c, s, 0] + step2[c, s]
            out_ref[:, cols] = (x1_ref[:, cols].astype(F32) + total).astype(BF16)

    def block_step(c, carry):
        slot = lax.rem(experts + c, SLOTS)

        @pl.when(c < blocks)
        def _():
            for e in range(experts):
                part_of, quarter = e // 4, e % 4
                if quarter == 0:
                    wait_weights(slot, part_of)
                down = ring[slot, part_of, (quarter // 2) * half_rows:(quarter // 2 + 1) * half_rows,
                            (quarter % 2) * bcols:(quarter % 2 + 1) * bcols]
                rows_out = jnp.dot(act[e * groups * CAP:(e + 1) * groups * CAP, :], down, preferred_element_type=F32).astype(BF16)
                for b in range(groups):
                    ybuf[b, e * CAP:(e + 1) * CAP, :] = rows_out[b * CAP:(b + 1) * CAP, :]

        @pl.when(jnp.logical_and(c >= 1, c <= blocks))
        def _():
            relay_pair(c - 1)

        @pl.when(c < blocks)
        def _():
            for m in range(chips):
                for k in range(2):
                    sums = jnp.dot(terms[2 * m + k], ybuf[2 * m + k], preferred_element_type=F32)
                    part[lax.rem(c, 2), m, k] = sums[:rows] + sums[rows:2 * rows] + sums[2 * rows:]
            pair_copy(c).start()

        @pl.when(jnp.logical_and(c >= 2, c <= blocks + 1))
        def _():
            relay_first(c - 2)

        @pl.when(c >= 3)
        def _():
            finish(c - 3)
        return carry

    lax.fori_loop(0, blocks + 3, block_step, 0)
    for copy in gates + ahead + passed:
        copy.wait_send()
    for r in (1, 2):
        for k in range(2):
            across(r, k).wait_send()
    for c in range(blocks):
        for s in range(2):
            for k in range(2):
                first_copy(c, s, k).wait_send()
            second_copy(c, s).wait_send()


def moe(h2, gt, x1, wg, wu, wd, groups):
    rows, dim = h2.shape
    experts, _, ffn = wg.shape
    slots = CAP * groups
    blocks = 4
    bcols = dim // blocks
    chips = groups // 2
    dma = pltpu.SemaphoreType.DMA
    return pl.pallas_call(
        moe_kernel,
        name="moe",
        out_shape=jax.ShapeDtypeStruct((rows, dim), BF16),
        in_specs=[ANY] * 6,
        out_specs=VMEM,
        scratch_shapes=[
            pltpu.VMEM(h2.shape, BF16),
            pltpu.VMEM(gt.shape, F32),
            pltpu.VMEM(x1.shape, BF16),
            pltpu.VMEM((SLOTS, 2, dim, ffn), BF16),
            pltpu.VMEM((rows * groups, dim), BF16),
            pltpu.VMEM((experts, slots, dim), BF16),
            pltpu.VMEM((experts * slots, ffn), BF16),
            pltpu.VMEM((groups, experts * CAP, bcols), BF16),
            pltpu.VMEM((chips, 2 * experts * CAP, 2 * rows), BF16),
            pltpu.VMEM((chips, experts * CAP, 2 * rows), F32),
            pltpu.VMEM((groups, 3 * rows, experts * CAP), BF16),
            pltpu.VMEM((2, chips, 2, rows, bcols), F32),
            pltpu.VMEM((blocks, chips, rows, bcols), F32),
            pltpu.VMEM((blocks, 2, chips, rows, bcols // 2), F32),
            pltpu.VMEM((blocks, 2, 2, rows, bcols // 2), F32),
            pltpu.VMEM((blocks, 2, rows, bcols // 2), F32),
            pltpu.VMEM((groups, experts, 2 * rows), F32),
            dma((3,)), dma((SLOTS, 2)),
            dma((2, 2)), dma((2, 2)), dma((2,)), dma((2,)), dma((4, 2)), dma((4, 2)), dma((8,)), dma((8,)),
            dma((blocks,)), dma((blocks,)), dma((blocks, 2, 2)), dma((blocks, 2, 2)), dma((blocks, 2)), dma((blocks, 2)),
        ],
        compiler_params=pltpu.CompilerParams(collective_id=0, has_side_effects=True, vmem_limit_bytes=62 * 2 ** 20),
    )(h2, gt, x1, wg, wu, wd)


def solution(mesh):
    groups = mesh.shape['ep']
    batch_axes = ('dp', 'ep')

    def device_step(hidden, positions, expert_ids, k_cache, v_cache, w_query, w_key, w_value, w_out, attn_gain, q_gain, k_gain, mlp_gain, w_router, w_gate, w_up, w_down):
        ids = jnp.transpose(expert_ids, (0, 2, 1))
        router_t = w_router.T
        caches = None
        for layer in range(expert_ids.shape[0]):
            x1, h2, gt, k_new, v_new = attention(layer, positions, hidden, ids, attn_gain, q_gain, k_gain, mlp_gain, router_t,
                                                 w_query, w_key, w_value, w_out, k_cache, v_cache, caches)
            caches = (k_new, v_new)
            hidden = moe(h2, gt, x1, w_gate, w_up, w_down, groups)
        return hidden, caches[0], caches[1]

    row_spec = P(batch_axes, None)
    cache_spec = P(None, batch_axes, None, None, None)
    full_spec = P()
    expert_spec = P('ep', None, None)
    in_specs = (row_spec, P(batch_axes), P(None, batch_axes, None), cache_spec, cache_spec, full_spec, full_spec, full_spec, full_spec, full_spec, full_spec, full_spec, full_spec, full_spec, expert_spec, expert_spec, expert_spec)
    return jax.shard_map(device_step, mesh=mesh, in_specs=in_specs, out_specs=(row_spec, cache_spec, cache_spec), check_vma=False)
```

```python
import functools
import math

import jax
import jax.numpy as jnp
from jax import lax
from jax.experimental import pallas as pl
from jax.experimental.pallas import tpu as pltpu
from jax.sharding import PartitionSpec as P

RMS_EPS = 1e-5
ROPE_BASE = 10000.0
CAP = 16
SLOTS = 6
FCOLS = 512
ACOLS = 512
MID = 4
LAG = 7
F32 = jnp.float32
BF16 = jnp.bfloat16
ANY = pl.BlockSpec(memory_space=pl.ANY)
VMEM = pl.BlockSpec(memory_space=pltpu.VMEM)
SMEM = pl.BlockSpec(memory_space=pltpu.SMEM)
MESH = pl.DeviceIdType.MESH
NT = (((1,), (1,)), ((), ()))


def rms_rows(values, gain_row):
    inv_rms = lax.rsqrt(jnp.mean(values * values, axis=-1, keepdims=True) + RMS_EPS)
    return values * inv_rms * gain_row


def attn_kernel(layer, pos_hbm, x_hbm, attn_gain_hbm, q_gain_hbm, k_gain_hbm,
                wq, wk, wv, wo, k_in, v_in, *rest):
    if layer > 0:
        rest = rest[2:]
    (x1_ref, k_out, v_out,
     pos_ref, x_ref, attn_gain, q_gain, k_gain, angle,
     wbuf, kbuf, vbuf, h_buf, lin, q2d, k2d, probs, mixed, ssem, wsem, csem, osem) = rest
    rows, dim = x_ref.shape
    heads, hd = k_in.shape[3], k_in.shape[4]
    cache_len = k_in.shape[2]
    half = dim // 2

    def wcopy(i):
        src = (wq, wk, wv, wo)[i // 2]
        return pltpu.make_async_copy(src.at[layer, :, pl.ds((i % 2) * half, half)], wbuf.at[i], wsem.at[i])

    kcopy = pltpu.make_async_copy(k_in.at[layer], kbuf, csem.at[0])
    vcopy = pltpu.make_async_copy(v_in.at[layer], vbuf, csem.at[1])
    small = [pltpu.make_async_copy(src, dst, ssem.at[n]) for n, (src, dst) in enumerate((
        (x_hbm, x_ref), (attn_gain_hbm, attn_gain), (pos_hbm, pos_ref), (q_gain_hbm, q_gain), (k_gain_hbm, k_gain)))]
    for copy in small:
        copy.start()
    for i in range(4):
        wcopy(i).start(priority=1)
    after = {0: [kcopy], 1: [wcopy(4)], 2: [wcopy(5)], 3: [vcopy], 4: [wcopy(6)], 5: [wcopy(7)]}
    for copy in small:
        copy.wait()
    x = x_ref[...].astype(F32)
    h_buf[...] = rms_rows(x, attn_gain[layer:layer + 1, :]).astype(BF16)
    lane = lax.broadcasted_iota(jnp.int32, (1, hd), 1)
    exponent = (lane % (hd // 2)).astype(F32) / (hd // 2)
    frequencies = jnp.exp(exponent * -math.log(ROPE_BASE))
    for b in range(rows):
        angle[b:b + 1, :] = frequencies * pos_ref[b].astype(F32)
    angles = angle[...]
    cos = jnp.cos(angles)
    sin = jnp.where(lane < hd // 2, -1.0, 1.0) * jnp.sin(angles)
    def project(which):
        for j in range(2):
            wcopy(2 * which + j).wait()
            for copy in after.get(2 * which + j, ()):
                copy.start(priority=1)
            for n in range(0, half, ACOLS):
                lin[:, j * half + n:j * half + n + ACOLS] = jnp.dot(
                    h_buf[...], wbuf[2 * which + j, :, n:n + ACOLS], preferred_element_type=F32)

    def spread(gain_ref, dst):
        values = lin[...]
        inv_rms = lax.rsqrt(jnp.mean(values * values, axis=-1, keepdims=True) + RMS_EPS)
        for h in range(heads):
            cols = slice(h * hd, (h + 1) * hd)
            part = lin[:, cols] * inv_rms * gain_ref[layer:layer + 1, cols]
            part = part * cos + pltpu.roll(part, hd // 2, 1) * sin
            dst[pl.ds(h, rows, stride=heads), :] = part

    project(0)
    spread(q_gain, q2d)
    project(1)
    spread(k_gain, k2d)
    kcopy.wait()

    span = cache_len * heads
    col = lax.broadcasted_iota(jnp.int32, (heads, span), 1)
    row = lax.broadcasted_iota(jnp.int32, (heads, span), 0)
    same_head = (col % heads) == row
    cache_row = jnp.where(same_head, col // heads, cache_len)
    scale = hd ** -0.5
    group = 8
    groups = rows // group

    def out_copy(which, g):
        at = pl.ds(pl.multiple_of(g * group, group), group)
        src, dst = ((kbuf, k_out), (vbuf, v_out))[which]
        return pltpu.make_async_copy(src.at[at], dst.at[layer, at], osem.at[which, g])

    def heads_of(b):
        return pl.ds(pl.multiple_of(b * heads, heads), heads)

    def score(g, carry):
        for i in range(group):
            b = g * group + i
            p = pos_ref[b]
            kbuf[b, p] = k2d[heads_of(b), :].astype(BF16)
            kmat = kbuf[b].reshape(span, hd)
            scores = lax.dot_general(q2d[heads_of(b), :].astype(BF16), kmat, NT, preferred_element_type=F32) * scale
            valid = cache_row <= p
            scores = jnp.where(valid, scores, -1e30)
            peak = jnp.max(scores, axis=-1, keepdims=True)
            weight = jnp.where(valid, jnp.exp(scores - peak), 0.0)
            probs[heads_of(b), :] = (weight / jnp.sum(weight, axis=-1, keepdims=True)).astype(BF16)

        @pl.when(g > 0)
        def _():
            out_copy(0, g - 1).start()
        return carry

    lax.fori_loop(0, groups, score, 0)
    project(2)
    out_copy(0, groups - 1).start()
    v2d = q2d
    o2d = k2d
    for h in range(heads):
        v2d[pl.ds(h, rows, stride=heads), :] = lin[:, h * hd:(h + 1) * hd]
    vcopy.wait()

    def mix(g, carry):
        for i in range(group):
            b = g * group + i
            vbuf[b, pos_ref[b]] = v2d[heads_of(b), :].astype(BF16)
            o2d[heads_of(b), :] = jnp.dot(probs[heads_of(b), :], vbuf[b].reshape(span, hd), preferred_element_type=F32)

        @pl.when(g > 0)
        def _():
            out_copy(1, g - 1).start()
        return carry

    lax.fori_loop(0, groups, mix, 0)
    for h in range(heads):
        mixed[:, h * hd:(h + 1) * hd] = o2d[pl.ds(h, rows, stride=heads), :].astype(BF16)
    out_copy(1, groups - 1).start()
    for j in range(2):
        cols = slice(j * half, (j + 1) * half)
        wcopy(6 + j).wait()
        lin[:, cols] = x_ref[:, cols].astype(F32) + jnp.dot(mixed[...], wbuf[6 + j], preferred_element_type=F32)
    x1_ref[...] = lin[...].astype(BF16)
    for g in range(groups):
        for which in range(2):
            out_copy(which, g).wait()


def attention(layer, pos, x, attn_gain, q_gain, k_gain, wq, wk, wv, wo, k_in, v_in, prev):
    rows, dim = x.shape
    _, _, cache_len, heads, hd = k_in.shape
    aliases = {} if prev is None else {11: 1, 12: 2}
    prev = () if prev is None else prev
    groups = rows // 8
    return pl.pallas_call(
        functools.partial(attn_kernel, layer),
        name="attn",
        out_shape=(
            jax.ShapeDtypeStruct((rows, dim), BF16),
            jax.ShapeDtypeStruct(k_in.shape, BF16),
            jax.ShapeDtypeStruct(v_in.shape, BF16),
        ),
        in_specs=[ANY] * (11 + len(prev)),
        out_specs=(VMEM, ANY, ANY),
        scratch_shapes=[
            pltpu.SMEM(pos.shape, pos.dtype),
            *[pltpu.VMEM(a.shape, a.dtype) for a in (x, attn_gain, q_gain, k_gain)],
            pltpu.VMEM((rows, hd), F32),
            pltpu.VMEM((8, dim, dim // 2), BF16),
            pltpu.VMEM(k_in.shape[1:], BF16),
            pltpu.VMEM(v_in.shape[1:], BF16),
            pltpu.VMEM((rows, dim), BF16),
            pltpu.VMEM((rows, dim), F32),
            pltpu.VMEM((rows * heads, hd), F32),
            pltpu.VMEM((rows * heads, hd), F32),
            pltpu.VMEM((rows * heads, cache_len * heads), BF16),
            pltpu.VMEM((rows, dim), BF16),
            pltpu.SemaphoreType.DMA((5,)),
            pltpu.SemaphoreType.DMA((8,)),
            pltpu.SemaphoreType.DMA((2,)),
            pltpu.SemaphoreType.DMA((2, groups)),
        ],
        input_output_aliases=aliases,
        compiler_params=pltpu.CompilerParams(vmem_limit_bytes=60 * 2 ** 20),
    )(pos, x, attn_gain, q_gain, k_gain, wq, wk, wv, wo, k_in, v_in, *prev)


def moe_kernel(layer, x1_hbm, mlp_gain_hbm, ids_hbm, router_hbm, wg, wu, wd, out_ref,
               x1_ref, mlp_gain, ids_ref, router_ref, gt_ref, ring, xall, xs, ybuf, pick, terms, part, dr, step1, step2, gtall,
               ssem, wsem, a_send, a_recv, f_send, f_recv, d_send, d_recv, g_send, g_recv, p_send, p_recv, u_send, u_recv, w_send, w_recv):
    rows, dim = x1_ref.shape
    experts, _, ffn = wg.shape
    all_experts = router_ref.shape[0]
    groups = xs.shape[1] // CAP
    chips = groups // 2
    bcols = ybuf.shape[2]
    blocks = dim // bcols
    sub = bcols // 2
    wcols = ring.shape[3] // 2
    per = wcols // bcols
    pairs = experts + dim // wcols
    half_rows = ring.shape[2] // 2
    hrows = rows // 2

    def start_experts(i, slot):
        pltpu.make_async_copy(wg.at[i], ring.at[slot, 0], wsem.at[slot, 0]).start(priority=1)
        pltpu.make_async_copy(wu.at[i], ring.at[slot, 1], wsem.at[slot, 1]).start(priority=1)

    def start_down(c, slot):
        cols = pl.ds(pl.multiple_of(c * wcols, wcols), wcols)
        for e in range(experts):
            part_of, quarter = e // 4, e % 4
            pltpu.make_async_copy(
                wd.at[e, :, cols],
                ring.at[slot, part_of, pl.ds((quarter // 2) * half_rows, half_rows), pl.ds((quarter % 2) * wcols, wcols)],
                wsem.at[slot, part_of]).start(priority=1)

    def wait_weights(slot, part_of):
        pltpu.make_async_copy(wg.at[0], ring.at[slot, part_of], wsem.at[slot, part_of]).wait()

    small = [pltpu.make_async_copy(src, dst, ssem.at[n]) for n, (src, dst) in enumerate((
        (x1_hbm, x1_ref), (mlp_gain_hbm, mlp_gain), (ids_hbm, ids_ref), (router_hbm, router_ref)))]
    for copy in small:
        copy.start()
    for i in range(SLOTS):
        start_experts(i, i)

    me = lax.axis_index("ep")
    core = lax.rem(me, 2)
    chip = lax.div(me, 2)
    at_x = lax.rem(chip, 2)
    at_y = lax.div(chip, 2)

    def chip_at(r):
        cx = 1 - at_x if r % 2 else at_x
        cy = 1 - at_y if r // 2 else at_y
        return 2 * cy + cx

    def device_at(q):
        return 2 * chip_at(q // 2) + (1 - core if q % 2 else core)

    barrier = pltpu.get_barrier_semaphore()
    for q in range(1, 8):
        pl.semaphore_signal(barrier, inc=1, device_id={"ep": device_at(q)}, device_id_type=MESH)
    for copy in small:
        copy.wait()
    h2 = rms_rows(x1_ref[...].astype(F32), mlp_gain[layer:layer + 1, :]).astype(BF16)
    xall[pl.ds(pl.multiple_of(me * rows, rows), rows), :] = h2
    expert_row = lax.broadcasted_iota(jnp.int32, (all_experts, 128), 0)
    wide_ids = jnp.concatenate([ids_ref[layer]] * (128 // rows), axis=1)
    hits = expert_row == wide_ids[0:1, :]
    for j in range(1, wide_ids.shape[0]):
        hits = jnp.logical_or(hits, expert_row == wide_ids[j:j + 1, :])
    member = jnp.where(hits, 1.0, 0.0)
    logits = lax.dot_general(router_ref[...], jnp.concatenate([h2] * (128 // rows), axis=0), NT, preferred_element_type=F32)
    logits = jnp.exp(logits - jnp.max(logits, axis=0, keepdims=True))
    router_probs = logits / jnp.sum(logits, axis=0, keepdims=True)
    gt_ref[...] = jnp.where(member > 0.5, router_probs, -1.0)
    pl.semaphore_wait(barrier, 7)

    def rows_of(dev):
        return pl.ds(pl.multiple_of(dev * rows, rows), rows)

    def half_of(dev, k):
        return pl.ds(pl.multiple_of(dev * rows + k * hrows, hrows), hrows)

    def experts_of(dev):
        return pl.ds(pl.multiple_of(dev * experts, experts), experts)

    def remote(src, dst, send, recv, dev):
        return pltpu.make_async_remote_copy(src_ref=src, dst_ref=dst, send_sem=send, recv_sem=recv,
                                            device_id={"ep": dev}, device_id_type=MESH)

    partner = device_at(1)
    gates = [remote(gt_ref.at[experts_of(device_at(q))], gtall.at[me], g_send.at[q], g_recv.at[q], device_at(q))
             for q in range(1, 8)]

    def across(r, k):
        return remote(xall.at[half_of(me, k)], xall.at[half_of(me, k)], a_send.at[r - 1, k], a_recv.at[r - 1, k],
                      device_at(2 * r))

    own = remote(xall.at[rows_of(me)], xall.at[rows_of(me)], d_send.at[0, 0], d_recv.at[0, 0], partner)
    for copy in gates:
        copy.start()
    for r, k in ((1, 0), (2, 1), (1, 1), (2, 0)):
        across(r, k).start()
    own.start()
    gtall[me] = gt_ref[experts_of(me), :]
    for copy in gates:
        copy.wait_recv()

    lane = lax.broadcasted_iota(jnp.int32, (experts, 2 * rows), 1)
    gate_rows = jnp.concatenate([jnp.where(lane < rows, gtall[2 * j], gtall[2 * j + 1]) for j in range(chips)], axis=0)
    chosen = gate_rows >= 0.0
    first = lax.broadcasted_iota(jnp.int32, (2 * rows, 2 * rows), 0)
    second = lax.broadcasted_iota(jnp.int32, (2 * rows, 2 * rows), 1)
    upper = jnp.logical_and(first <= second, first // rows == second // rows)
    counted = jnp.dot(jnp.where(chosen, 1.0, 0.0).astype(BF16), jnp.where(upper, 1.0, 0.0).astype(BF16),
                      preferred_element_type=F32)
    ranks = jnp.where(chosen, counted - 1.0, -1.0)
    slot_of = lax.broadcasted_iota(jnp.int32, (CAP, 2 * rows), 0).astype(F32)
    left = lax.broadcasted_iota(jnp.int32, (CAP, 2 * rows), 1) < rows
    width = experts * CAP
    for j in range(chips):
        for e in range(experts):
            line = slice(j * experts + e, j * experts + e + 1)
            hit = slot_of == ranks[line, :]
            at = slice(e * CAP, (e + 1) * CAP)
            pick[j, at, :] = jnp.where(jnp.logical_and(hit, left), 1.0, 0.0).astype(BF16)
            pick[j, width + e * CAP:width + (e + 1) * CAP, :] = jnp.where(
                jnp.logical_and(hit, jnp.logical_not(left)), 1.0, 0.0).astype(BF16)
            part[0, 0, e * CAP // rows, j, e * CAP % rows:e * CAP % rows + CAP, :] = jnp.where(hit, gate_rows[line, :], 0.0)
    for j in range(chips):
        gated = jnp.transpose(jnp.concatenate([part[0, 0, 0, j], part[0, 0, 1, j]], axis=0))
        high = gated.astype(BF16)
        rest = gated - high.astype(F32)
        middle = rest.astype(BF16)
        low = (rest - middle.astype(F32)).astype(BF16)
        for k in range(2):
            for n, term in enumerate((high, middle, low)):
                terms[2 * j + k, n * rows:(n + 1) * rows, :] = term[k * rows:(k + 1) * rows, :]

    passed = [own]

    def hand_over(r, k):
        block = xall.at[half_of(device_at(2 * r), k)]
        copy = remote(block, block, d_send.at[r, k], d_recv.at[r, k], partner)
        copy.start()
        passed.append(copy)

    def forward(r, k):
        block = xall.at[half_of(device_at(2 * r), k)]
        return remote(block, block, f_send.at[k], f_recv.at[k], device_at(2 * (3 - r)))

    across(1, 0).wait_recv()
    ahead = [forward(1, 0)]
    ahead[0].start()
    hand_over(1, 0)
    across(2, 1).wait_recv()
    ahead.append(forward(2, 1))
    ahead[1].start()
    hand_over(2, 1)

    def take_rows(r):
        j = chip_at(r)
        chosen_rows = jnp.dot(pick[j], xall[pl.ds(pl.multiple_of(j * 2 * rows, 2 * rows), 2 * rows), :],
                              preferred_element_type=F32).astype(BF16)
        for k in range(2):
            for e in range(experts):
                xs[e + 1, pl.ds(pl.multiple_of((2 * j + k) * CAP, CAP), CAP), :] = chosen_rows[k * width + e * CAP:k * width + (e + 1) * CAP, :]

    own.wait_recv()
    take_rows(0)
    across(1, 1).wait_recv()
    hand_over(1, 1)
    across(2, 0).wait_recv()
    hand_over(2, 0)
    passed[1].wait_recv()
    passed[3].wait_recv()
    take_rows(1)
    passed[2].wait_recv()
    passed[4].wait_recv()
    take_rows(2)
    for k in range(2):
        ahead[k].wait_recv()
        hand_over(3, k)
    passed[5].wait_recv()
    passed[6].wait_recv()
    take_rows(3)

    def expert_step(e, carry):
        slot = lax.rem(e, SLOTS)
        wait_weights(slot, 0)
        wait_weights(slot, 1)
        for n in range(ffn // FCOLS):
            cols = slice(n * FCOLS, (n + 1) * FCOLS)
            gate_act = jnp.dot(xs[e + 1], ring[slot, 0, :, cols], preferred_element_type=F32)
            up_act = jnp.dot(xs[e + 1], ring[slot, 1, :, cols], preferred_element_type=F32)
            xs[e, :, cols] = (jax.nn.silu(gate_act) * up_act).astype(BF16)

        @pl.when(e + SLOTS < experts)
        def _():
            start_experts(e + SLOTS, slot)

        @pl.when(jnp.logical_and(e + SLOTS >= experts, e + SLOTS < pairs))
        def _():
            start_down(e + SLOTS - experts, slot)
        return carry

    lax.fori_loop(0, experts, expert_step, 0)

    def pair_copy(c):
        return remote(part.at[lax.rem(c, 2), 1 - core], dr.at[c], p_send.at[c], p_recv.at[c], partner)

    def first_copy(c, s, k):
        to = 1 + s
        return remote(dr.at[c, s, chip_at((to, 3)[k])], step1.at[c, s, k], u_send.at[c, s, k], u_recv.at[c, s, k],
                      device_at(2 * to))

    def second_copy(c, s):
        to = 2 - s
        return remote(dr.at[c, s, chip_at(to)], step2.at[c, s], w_send.at[c, s], w_recv.at[c, s], device_at(2 * to))

    def relay_pair(c):
        copy = pair_copy(c)
        copy.wait_send()
        copy.wait_recv()
        dr[c] = dr[c] + part[lax.rem(c, 2), core]
        for k in (1, 0):
            for s in range(2):
                first_copy(c, s, k).start()

    def relay_first(c):
        for s in range(2):
            first_copy(c, s, 1).wait_recv()
            to = chip_at(2 - s)
            dr[c, s, to] = dr[c, s, to] + step1[c, s, 1]
            second_copy(c, s).start()

    def finish(c):
        for s in range(2):
            first_copy(c, s, 0).wait_recv()
            second_copy(c, s).wait_recv()
            cols = pl.ds(pl.multiple_of(c * bcols + s * sub, sub), sub)
            total = dr[c, s, chip] + step1[c, s, 0] + step2[c, s]
            out_ref[:, cols] = (x1_ref[:, cols].astype(F32) + total).astype(out_ref.dtype)

    def block_step(c, carry):
        slot = lax.rem(experts + lax.div(c, per), SLOTS)
        shift = lax.rem(c, per) * bcols

        @pl.when(c < blocks)
        def _():
            for e in range(experts):
                part_of, quarter = e // 4, e % 4
                if quarter == 0:
                    @pl.when(shift == 0)
                    def _():
                        wait_weights(slot, part_of)
                down = ring[slot, part_of, (quarter // 2) * half_rows:(quarter // 2 + 1) * half_rows,
                            pl.ds(pl.multiple_of((quarter % 2) * wcols + shift, bcols), bcols)]
                rows_out = jnp.dot(xs[e, :, :ffn], down, preferred_element_type=F32).astype(BF16)
                for b in range(groups):
                    ybuf[b, e * CAP:(e + 1) * CAP, :] = rows_out[b * CAP:(b + 1) * CAP, :]

        @pl.when(jnp.logical_and(c >= 1, c <= blocks))
        def _():
            relay_pair(c - 1)

        @pl.when(c < blocks)
        def _():
            for m in range(chips):
                for k in range(2):
                    sums = jnp.dot(terms[2 * m + k], ybuf[2 * m + k], preferred_element_type=F32)
                    sums = sums[:rows] + sums[rows:2 * rows] + sums[2 * rows:]
                    for s in range(2):
                        part[lax.rem(c, 2), k, s, m] = sums[:, s * sub:(s + 1) * sub]
            pair_copy(c).start()

        @pl.when(jnp.logical_and(c >= MID, c < blocks + MID))
        def _():
            relay_first(c - MID)

        @pl.when(c >= LAG)
        def _():
            finish(c - LAG)
        return carry

    lax.fori_loop(0, blocks + LAG, block_step, 0)
    for copy in gates + ahead + passed:
        copy.wait_send()
    for r in (1, 2):
        for k in range(2):
            across(r, k).wait_send()
    for c in range(blocks):
        for s in range(2):
            for k in range(2):
                first_copy(c, s, k).wait_send()
            second_copy(c, s).wait_send()


def moe(layer, x1, mlp_gain, ids, router_t, wg, wu, wd, groups, out_type):
    rows, dim = x1.shape
    experts, _, ffn = wg.shape
    slots = CAP * groups
    blocks = 8
    bcols = dim // blocks
    chips = groups // 2
    dma = pltpu.SemaphoreType.DMA
    return pl.pallas_call(
        functools.partial(moe_kernel, layer),
        name="moe",
        out_shape=jax.ShapeDtypeStruct((rows, dim), out_type),
        in_specs=[ANY] * 7,
        out_specs=VMEM,
        scratch_shapes=[
            *[pltpu.VMEM(a.shape, a.dtype) for a in (x1, mlp_gain, ids, router_t)],
            pltpu.VMEM((router_t.shape[0], 128), F32),
            pltpu.VMEM((SLOTS, 2, dim, ffn), BF16),
            pltpu.VMEM((rows * groups, dim), BF16),
            pltpu.VMEM((experts + 1, slots, dim), BF16),
            pltpu.VMEM((groups, experts * CAP, bcols), BF16),
            pltpu.VMEM((chips, 2 * experts * CAP, 2 * rows), BF16),
            pltpu.VMEM((groups, 3 * rows, experts * CAP), BF16),
            pltpu.VMEM((2, 2, 2, chips, rows, bcols // 2), F32),
            pltpu.VMEM((blocks, 2, chips, rows, bcols // 2), F32),
            pltpu.VMEM((blocks, 2, 2, rows, bcols // 2), F32),
            pltpu.VMEM((blocks, 2, rows, bcols // 2), F32),
            pltpu.VMEM((groups, experts, 2 * rows), F32),
            dma((4,)), dma((SLOTS, 2)),
            dma((2, 2)), dma((2, 2)), dma((2,)), dma((2,)), dma((4, 2)), dma((4, 2)), dma((8,)), dma((8,)),
            dma((blocks,)), dma((blocks,)), dma((blocks, 2, 2)), dma((blocks, 2, 2)), dma((blocks, 2)), dma((blocks, 2)),
        ],
        compiler_params=pltpu.CompilerParams(collective_id=layer, has_side_effects=True, vmem_limit_bytes=67043328),
    )(x1, mlp_gain, ids, router_t, wg, wu, wd)


def solution(mesh):
    groups = mesh.shape['ep']
    batch_axes = ('dp', 'ep')

    def device_step(hidden, positions, expert_ids, k_cache, v_cache, w_query, w_key, w_value, w_out, attn_gain, q_gain, k_gain, mlp_gain, w_router, w_gate, w_up, w_down):
        ids = jnp.transpose(expert_ids, (0, 2, 1))
        router_t = w_router.T
        caches = None
        for layer in range(expert_ids.shape[0]):
            x1, k_new, v_new = attention(layer, positions, hidden, attn_gain, q_gain, k_gain,
                                         w_query, w_key, w_value, w_out, k_cache, v_cache, caches)
            caches = (k_new, v_new)
            out_type = BF16
            hidden = moe(layer, x1, mlp_gain, ids, router_t, w_gate, w_up, w_down, groups, out_type)
        return hidden.astype(BF16), caches[0], caches[1]

    row_spec = P(batch_axes, None)
    cache_spec = P(None, batch_axes, None, None, None)
    full_spec = P()
    expert_spec = P('ep', None, None)
    in_specs = (row_spec, P(batch_axes), P(None, batch_axes, None), cache_spec, cache_spec, full_spec, full_spec, full_spec, full_spec, full_spec, full_spec, full_spec, full_spec, full_spec, expert_spec, expert_spec, expert_spec)
    return jax.shard_map(device_step, mesh=mesh, in_specs=in_specs, out_specs=(row_spec, cache_spec, cache_spec), check_vma=False)
```

```python
import functools
import math

import jax
import jax.numpy as jnp
from jax import lax
from jax.experimental import pallas as pl
from jax.experimental.pallas import tpu as pltpu
from jax.sharding import PartitionSpec as P

RMS_EPS = 1e-5
ROPE_BASE = 10000.0
CAP = 16
SLOTS = 6
FCOLS = 512
ACOLS = 512
MID = 4
LAG = 7
F32 = jnp.float32
BF16 = jnp.bfloat16
ANY = pl.BlockSpec(memory_space=pl.ANY)
VMEM = pl.BlockSpec(memory_space=pltpu.VMEM)
SMEM = pl.BlockSpec(memory_space=pltpu.SMEM)
MESH = pl.DeviceIdType.MESH
NT = (((1,), (1,)), ((), ()))


def rms_rows(values, gain_row):
    inv_rms = lax.rsqrt(jnp.mean(values * values, axis=-1, keepdims=True) + RMS_EPS)
    return values * inv_rms * gain_row


def rotary(angle, pos_ref, rows, hd):
    lane = lax.broadcasted_iota(jnp.int32, (1, hd), 1)
    exponent = (lane % (hd // 2)).astype(F32) / (hd // 2)
    frequencies = jnp.exp(exponent * -math.log(ROPE_BASE))
    for b in range(rows):
        angle[b:b + 1, :] = frequencies * pos_ref[b].astype(F32)
    angles = angle[...]
    return jnp.cos(angles), jnp.where(lane < hd // 2, -1.0, 1.0) * jnp.sin(angles)


def attn_kernel(layer, ready, pos_hbm, x_hbm, attn_gain_hbm, q_gain_hbm, k_gain_hbm,
                wq, wk, wv, wo, k_in, v_in, *rest):
    if layer > 0:
        rest = rest[2:]
    if ready:
        qkv_hbm, *rest = rest
    (x1_ref, k_out, v_out,
     qkv, pos_ref, x_ref, attn_gain, q_gain, k_gain, angle,
     wbuf, kbuf, vbuf, h_buf, lin, q2d, k2d, probs, mixed, ssem, wsem, csem, osem) = rest
    rows, dim = x_ref.shape
    heads, hd = k_in.shape[3], k_in.shape[4]
    cache_len = k_in.shape[2]
    half = dim // 2

    def wcopy(i):
        src = (wq, wk, wv, wo)[i // 2]
        return pltpu.make_async_copy(src.at[layer, :, pl.ds((i % 2) * half, half)], wbuf.at[i], wsem.at[i])

    kcopy = pltpu.make_async_copy(k_in.at[layer], kbuf, csem.at[0])
    vcopy = pltpu.make_async_copy(v_in.at[layer], vbuf, csem.at[1])
    small = [pltpu.make_async_copy(src, dst, ssem.at[n]) for n, (src, dst) in enumerate((
        (x_hbm, x_ref), (pos_hbm, pos_ref), *([(qkv_hbm, qkv)] if ready else [
            (attn_gain_hbm, attn_gain), (q_gain_hbm, q_gain), (k_gain_hbm, k_gain)])))]
    for copy in small:
        copy.start()
    if ready:
        kcopy.start()
        for copy in (vcopy, wcopy(6), wcopy(7)):
            copy.start(priority=1)
    else:
        for i in range(4):
            wcopy(i).start(priority=1)
    after = {} if ready else {0: [kcopy], 1: [wcopy(4)], 2: [wcopy(5)], 3: [vcopy], 4: [wcopy(6)], 5: [wcopy(7)]}
    for copy in small:
        copy.wait()
    if not ready:
        x = x_ref[...].astype(F32)
        h_buf[...] = rms_rows(x, attn_gain[layer:layer + 1, :]).astype(BF16)
    cos, sin = (None, None) if ready else rotary(angle, pos_ref, rows, hd)

    def project(which):
        for j in range(2):
            wcopy(2 * which + j).wait()
            for copy in after.get(2 * which + j, ()):
                copy.start(priority=1)
            for n in range(0, half, ACOLS):
                lin[:, j * half + n:j * half + n + ACOLS] = jnp.dot(
                    h_buf[...], wbuf[2 * which + j, :, n:n + ACOLS], preferred_element_type=F32)

    def spread(gain_ref, dst):
        values = lin[...]
        inv_rms = lax.rsqrt(jnp.mean(values * values, axis=-1, keepdims=True) + RMS_EPS)
        for h in range(heads):
            cols = slice(h * hd, (h + 1) * hd)
            part = lin[:, cols] * inv_rms * gain_ref[layer:layer + 1, cols]
            part = part * cos + pltpu.roll(part, hd // 2, 1) * sin
            dst[pl.ds(h, rows, stride=heads), :] = part

    def arrange(which, dst):
        for h in range(heads):
            dst[pl.ds(h, rows, stride=heads), :] = qkv[which, :, h * hd:(h + 1) * hd].astype(F32)

    if ready:
        arrange(0, q2d)
        arrange(1, k2d)
    else:
        project(0)
        spread(q_gain, q2d)
        project(1)
        spread(k_gain, k2d)
    kcopy.wait()

    span = cache_len * heads
    col = lax.broadcasted_iota(jnp.int32, (heads, span), 1)
    row = lax.broadcasted_iota(jnp.int32, (heads, span), 0)
    same_head = (col % heads) == row
    cache_row = jnp.where(same_head, col // heads, cache_len)
    scale = hd ** -0.5
    group = 8
    groups = rows // group

    def out_copy(which, g):
        at = pl.ds(pl.multiple_of(g * group, group), group)
        src, dst = ((kbuf, k_out), (vbuf, v_out))[which]
        return pltpu.make_async_copy(src.at[at], dst.at[layer, at], osem.at[which, g])

    def heads_of(b):
        return pl.ds(pl.multiple_of(b * heads, heads), heads)

    def score(g, carry):
        for i in range(group):
            b = g * group + i
            p = pos_ref[b]
            kbuf[b, p] = k2d[heads_of(b), :].astype(BF16)
            kmat = kbuf[b].reshape(span, hd)
            scores = lax.dot_general(q2d[heads_of(b), :].astype(BF16), kmat, NT, preferred_element_type=F32) * scale
            valid = cache_row <= p
            scores = jnp.where(valid, scores, -1e30)
            peak = jnp.max(scores, axis=-1, keepdims=True)
            weight = jnp.where(valid, jnp.exp(scores - peak), 0.0)
            probs[heads_of(b), :] = (weight / jnp.sum(weight, axis=-1, keepdims=True)).astype(BF16)

        @pl.when(g > 0)
        def _():
            out_copy(0, g - 1).start()
        return carry

    lax.fori_loop(0, groups, score, 0)
    v2d = q2d
    o2d = k2d
    if ready:
        arrange(2, v2d)
    else:
        project(2)
        for h in range(heads):
            v2d[pl.ds(h, rows, stride=heads), :] = lin[:, h * hd:(h + 1) * hd]
    out_copy(0, groups - 1).start()
    vcopy.wait()

    def mix(g, carry):
        for i in range(group):
            b = g * group + i
            vbuf[b, pos_ref[b]] = v2d[heads_of(b), :].astype(BF16)
            o2d[heads_of(b), :] = jnp.dot(probs[heads_of(b), :], vbuf[b].reshape(span, hd), preferred_element_type=F32)

        @pl.when(g > 0)
        def _():
            out_copy(1, g - 1).start()
        return carry

    lax.fori_loop(0, groups, mix, 0)
    for h in range(heads):
        mixed[:, h * hd:(h + 1) * hd] = o2d[pl.ds(h, rows, stride=heads), :].astype(BF16)
    out_copy(1, groups - 1).start()
    for j in range(2):
        cols = slice(j * half, (j + 1) * half)
        wcopy(6 + j).wait()
        lin[:, cols] = x_ref[:, cols].astype(F32) + jnp.dot(mixed[...], wbuf[6 + j], preferred_element_type=F32)
    x1_ref[...] = lin[...].astype(BF16)
    for g in range(groups):
        for which in range(2):
            out_copy(which, g).wait()


def attention(layer, pos, x, attn_gain, q_gain, k_gain, wq, wk, wv, wo, k_in, v_in, prev, ready):
    rows, dim = x.shape
    _, _, cache_len, heads, hd = k_in.shape
    aliases = {} if prev is None else {11: 1, 12: 2}
    prev = () if prev is None else prev
    groups = rows // 8
    return pl.pallas_call(
        functools.partial(attn_kernel, layer, bool(ready)),
        name="attn",
        out_shape=(
            jax.ShapeDtypeStruct((rows, dim), BF16),
            jax.ShapeDtypeStruct(k_in.shape, BF16),
            jax.ShapeDtypeStruct(v_in.shape, BF16),
        ),
        in_specs=[ANY] * (11 + len(prev) + len(ready)),
        out_specs=(VMEM, ANY, ANY),
        scratch_shapes=[
            pltpu.VMEM((3, rows, dim), BF16),
            pltpu.SMEM(pos.shape, pos.dtype),
            *[pltpu.VMEM(a.shape, a.dtype) for a in (x, attn_gain, q_gain, k_gain)],
            pltpu.VMEM((rows, hd), F32),
            pltpu.VMEM((8, dim, dim // 2), BF16),
            pltpu.VMEM(k_in.shape[1:], BF16),
            pltpu.VMEM(v_in.shape[1:], BF16),
            pltpu.VMEM((rows, dim), BF16),
            pltpu.VMEM((rows, dim), F32),
            pltpu.VMEM((rows * heads, hd), F32),
            pltpu.VMEM((rows * heads, hd), F32),
            pltpu.VMEM((rows * heads, cache_len * heads), BF16),
            pltpu.VMEM((rows, dim), BF16),
            pltpu.SemaphoreType.DMA((5,)),
            pltpu.SemaphoreType.DMA((8,)),
            pltpu.SemaphoreType.DMA((2,)),
            pltpu.SemaphoreType.DMA((2, groups)),
        ],
        input_output_aliases=aliases,
        compiler_params=pltpu.CompilerParams(vmem_limit_bytes=60 * 2 ** 20),
    )(pos, x, attn_gain, q_gain, k_gain, wq, wk, wv, wo, k_in, v_in, *prev, *ready)


def moe_kernel(layer, follow, x1_hbm, mlp_gain_hbm, ids_hbm, router_hbm, wg, wu, wd, *rest):
    if follow:
        (pos_hbm, attn_gain_hbm, q_gain_hbm, k_gain_hbm, wq, wk, wv, out_ref, qkv_out,
         pos_ref, attn_gain, q_gain, k_gain, angle, qsem, *rest) = rest
    else:
        out_ref, *rest = rest
    (x1_ref, mlp_gain, ids_ref, router_ref, gt_ref, ring, xall, xs, ybuf, pick, terms, part, dr, step1, step2, gtall,
               ssem, wsem, a_send, a_recv, f_send, f_recv, d_send, d_recv, g_send, g_recv, p_send, p_recv, u_send, u_recv, w_send, w_recv) = rest
    rows, dim = x1_ref.shape
    experts, _, ffn = wg.shape
    all_experts = router_ref.shape[0]
    groups = xs.shape[1] // CAP
    chips = groups // 2
    bcols = ybuf.shape[2]
    blocks = dim // bcols
    sub = bcols // 2
    wcols = ring.shape[3] // 2
    per = wcols // bcols
    pairs = experts + dim // wcols
    half_rows = ring.shape[2] // 2
    hrows = rows // 2

    def start_experts(i, slot):
        pltpu.make_async_copy(wg.at[i], ring.at[slot, 0], wsem.at[slot, 0]).start(priority=1)
        pltpu.make_async_copy(wu.at[i], ring.at[slot, 1], wsem.at[slot, 1]).start(priority=1)

    def start_down(c, slot):
        cols = pl.ds(pl.multiple_of(c * wcols, wcols), wcols)
        for e in range(experts):
            part_of, quarter = e // 4, e % 4
            pltpu.make_async_copy(
                wd.at[e, :, cols],
                ring.at[slot, part_of, pl.ds((quarter // 2) * half_rows, half_rows), pl.ds((quarter % 2) * wcols, wcols)],
                wsem.at[slot, part_of]).start(priority=1)

    def wait_weights(slot, part_of):
        pltpu.make_async_copy(wg.at[0], ring.at[slot, part_of], wsem.at[slot, part_of]).wait()

    if follow:
        late = [pltpu.make_async_copy(src, dst, qsem.at[n]) for n, (src, dst) in enumerate((
            (pos_hbm, pos_ref), (attn_gain_hbm, attn_gain), (q_gain_hbm, q_gain), (k_gain_hbm, k_gain)))]
        projections = (wq, wk, wv)

    def start_projection(which, slot):
        for j in range(2):
            cols = pl.ds(j * ffn, ffn)
            pltpu.make_async_copy(projections[which].at[layer + 1, :, cols], ring.at[slot, j], wsem.at[slot, j]).start(priority=1)

    small = [pltpu.make_async_copy(src, dst, ssem.at[n]) for n, (src, dst) in enumerate((
        (x1_hbm, x1_ref), (mlp_gain_hbm, mlp_gain), (ids_hbm, ids_ref), (router_hbm, router_ref)))]
    for copy in small:
        copy.start()
    if follow:
        for copy in late:
            copy.start()
    for i in range(SLOTS):
        start_experts(i, i)

    me = lax.axis_index("ep")
    core = lax.rem(me, 2)
    chip = lax.div(me, 2)
    at_x = lax.rem(chip, 2)
    at_y = lax.div(chip, 2)

    def chip_at(r):
        cx = 1 - at_x if r % 2 else at_x
        cy = 1 - at_y if r // 2 else at_y
        return 2 * cy + cx

    def device_at(q):
        return 2 * chip_at(q // 2) + (1 - core if q % 2 else core)

    barrier = pltpu.get_barrier_semaphore()
    for q in range(1, 8):
        pl.semaphore_signal(barrier, inc=1, device_id={"ep": device_at(q)}, device_id_type=MESH)
    for copy in small:
        copy.wait()
    h2 = rms_rows(x1_ref[...].astype(F32), mlp_gain[layer:layer + 1, :]).astype(BF16)
    xall[pl.ds(pl.multiple_of(me * rows, rows), rows), :] = h2
    expert_row = lax.broadcasted_iota(jnp.int32, (all_experts, 128), 0)
    wide_ids = jnp.concatenate([ids_ref[layer]] * (128 // rows), axis=1)
    hits = expert_row == wide_ids[0:1, :]
    for j in range(1, wide_ids.shape[0]):
        hits = jnp.logical_or(hits, expert_row == wide_ids[j:j + 1, :])
    member = jnp.where(hits, 1.0, 0.0)
    logits = lax.dot_general(router_ref[...], jnp.concatenate([h2] * (128 // rows), axis=0), NT, preferred_element_type=F32)
    logits = jnp.exp(logits - jnp.max(logits, axis=0, keepdims=True))
    router_probs = logits / jnp.sum(logits, axis=0, keepdims=True)
    gt_ref[...] = jnp.where(member > 0.5, router_probs, -1.0)
    pl.semaphore_wait(barrier, 7)

    def rows_of(dev):
        return pl.ds(pl.multiple_of(dev * rows, rows), rows)

    def half_of(dev, k):
        return pl.ds(pl.multiple_of(dev * rows + k * hrows, hrows), hrows)

    def experts_of(dev):
        return pl.ds(pl.multiple_of(dev * experts, experts), experts)

    def remote(src, dst, send, recv, dev):
        return pltpu.make_async_remote_copy(src_ref=src, dst_ref=dst, send_sem=send, recv_sem=recv,
                                            device_id={"ep": dev}, device_id_type=MESH)

    partner = device_at(1)
    gates = [remote(gt_ref.at[experts_of(device_at(q))], gtall.at[me], g_send.at[q], g_recv.at[q], device_at(q))
             for q in range(1, 8)]

    def across(r, k):
        return remote(xall.at[half_of(me, k)], xall.at[half_of(me, k)], a_send.at[r - 1, k], a_recv.at[r - 1, k],
                      device_at(2 * r))

    own = remote(xall.at[rows_of(me)], xall.at[rows_of(me)], d_send.at[0, 0], d_recv.at[0, 0], partner)
    for copy in gates:
        copy.start()
    for r, k in ((1, 0), (2, 1), (1, 1), (2, 0)):
        across(r, k).start()
    own.start()
    gtall[me] = gt_ref[experts_of(me), :]
    for copy in gates:
        copy.wait_recv()

    lane = lax.broadcasted_iota(jnp.int32, (experts, 2 * rows), 1)
    gate_rows = jnp.concatenate([jnp.where(lane < rows, gtall[2 * j], gtall[2 * j + 1]) for j in range(chips)], axis=0)
    chosen = gate_rows >= 0.0
    first = lax.broadcasted_iota(jnp.int32, (2 * rows, 2 * rows), 0)
    second = lax.broadcasted_iota(jnp.int32, (2 * rows, 2 * rows), 1)
    upper = jnp.logical_and(first <= second, first // rows == second // rows)
    counted = jnp.dot(jnp.where(chosen, 1.0, 0.0).astype(BF16), jnp.where(upper, 1.0, 0.0).astype(BF16),
                      preferred_element_type=F32)
    ranks = jnp.where(chosen, counted - 1.0, -1.0)
    slot_of = lax.broadcasted_iota(jnp.int32, (CAP, 2 * rows), 0).astype(F32)
    left = lax.broadcasted_iota(jnp.int32, (CAP, 2 * rows), 1) < rows
    width = experts * CAP
    for j in range(chips):
        for e in range(experts):
            line = slice(j * experts + e, j * experts + e + 1)
            hit = slot_of == ranks[line, :]
            at = slice(e * CAP, (e + 1) * CAP)
            pick[j, at, :] = jnp.where(jnp.logical_and(hit, left), 1.0, 0.0).astype(BF16)
            pick[j, width + e * CAP:width + (e + 1) * CAP, :] = jnp.where(
                jnp.logical_and(hit, jnp.logical_not(left)), 1.0, 0.0).astype(BF16)
            part[0, 0, e * CAP // rows, j, e * CAP % rows:e * CAP % rows + CAP, :] = jnp.where(hit, gate_rows[line, :], 0.0)
    for j in range(chips):
        gated = jnp.transpose(jnp.concatenate([part[0, 0, 0, j], part[0, 0, 1, j]], axis=0))
        high = gated.astype(BF16)
        rest = gated - high.astype(F32)
        middle = rest.astype(BF16)
        low = (rest - middle.astype(F32)).astype(BF16)
        for k in range(2):
            for n, term in enumerate((high, middle, low)):
                terms[2 * j + k, n * rows:(n + 1) * rows, :] = term[k * rows:(k + 1) * rows, :]

    passed = [own]

    def hand_over(r, k):
        block = xall.at[half_of(device_at(2 * r), k)]
        copy = remote(block, block, d_send.at[r, k], d_recv.at[r, k], partner)
        copy.start()
        passed.append(copy)

    def forward(r, k):
        block = xall.at[half_of(device_at(2 * r), k)]
        return remote(block, block, f_send.at[k], f_recv.at[k], device_at(2 * (3 - r)))

    across(1, 0).wait_recv()
    ahead = [forward(1, 0)]
    ahead[0].start()
    hand_over(1, 0)
    across(2, 1).wait_recv()
    ahead.append(forward(2, 1))
    ahead[1].start()
    hand_over(2, 1)

    def take_rows(r):
        j = chip_at(r)
        chosen_rows = jnp.dot(pick[j], xall[pl.ds(pl.multiple_of(j * 2 * rows, 2 * rows), 2 * rows), :],
                              preferred_element_type=F32).astype(BF16)
        for k in range(2):
            for e in range(experts):
                xs[e + 1, pl.ds(pl.multiple_of((2 * j + k) * CAP, CAP), CAP), :] = chosen_rows[k * width + e * CAP:k * width + (e + 1) * CAP, :]

    own.wait_recv()
    take_rows(0)
    across(1, 1).wait_recv()
    hand_over(1, 1)
    across(2, 0).wait_recv()
    hand_over(2, 0)
    passed[1].wait_recv()
    passed[3].wait_recv()
    take_rows(1)
    passed[2].wait_recv()
    passed[4].wait_recv()
    take_rows(2)
    for k in range(2):
        ahead[k].wait_recv()
        hand_over(3, k)
    passed[5].wait_recv()
    passed[6].wait_recv()
    take_rows(3)

    def expert_step(e, carry):
        slot = lax.rem(e, SLOTS)
        wait_weights(slot, 0)
        wait_weights(slot, 1)
        for n in range(ffn // FCOLS):
            cols = slice(n * FCOLS, (n + 1) * FCOLS)
            gate_act = jnp.dot(xs[e + 1], ring[slot, 0, :, cols], preferred_element_type=F32)
            up_act = jnp.dot(xs[e + 1], ring[slot, 1, :, cols], preferred_element_type=F32)
            xs[e, :, cols] = (jax.nn.silu(gate_act) * up_act).astype(BF16)

        @pl.when(e + SLOTS < experts)
        def _():
            start_experts(e + SLOTS, slot)

        @pl.when(jnp.logical_and(e + SLOTS >= experts, e + SLOTS < pairs))
        def _():
            start_down(e + SLOTS - experts, slot)

        if follow:
            for which in range(2):
                @pl.when(e + SLOTS == pairs + which)
                def _():
                    start_projection(which, slot)
        return carry

    lax.fori_loop(0, experts, expert_step, 0)

    def pair_copy(c):
        return remote(part.at[lax.rem(c, 2), 1 - core], dr.at[c], p_send.at[c], p_recv.at[c], partner)

    def first_copy(c, s, k):
        to = 1 + s
        return remote(dr.at[c, s, chip_at((to, 3)[k])], step1.at[c, s, k], u_send.at[c, s, k], u_recv.at[c, s, k],
                      device_at(2 * to))

    def second_copy(c, s):
        to = 2 - s
        return remote(dr.at[c, s, chip_at(to)], step2.at[c, s], w_send.at[c, s], w_recv.at[c, s], device_at(2 * to))

    def relay_pair(c):
        copy = pair_copy(c)
        copy.wait_send()
        copy.wait_recv()
        dr[c] = dr[c] + part[lax.rem(c, 2), core]
        for k in (1, 0):
            for s in range(2):
                first_copy(c, s, k).start()

    def relay_first(c):
        for s in range(2):
            first_copy(c, s, 1).wait_recv()
            to = chip_at(2 - s)
            dr[c, s, to] = dr[c, s, to] + step1[c, s, 1]
            second_copy(c, s).start()

    def finish(c):
        for s in range(2):
            first_copy(c, s, 0).wait_recv()
            second_copy(c, s).wait_recv()
            cols = pl.ds(pl.multiple_of(c * bcols + s * sub, sub), sub)
            total = dr[c, s, chip] + step1[c, s, 0] + step2[c, s]
            out_ref[:, cols] = (x1_ref[:, cols].astype(F32) + total).astype(out_ref.dtype)

    def block_step(c, carry):
        slot = lax.rem(experts + lax.div(c, per), SLOTS)
        shift = lax.rem(c, per) * bcols

        @pl.when(c < blocks)
        def _():
            for e in range(experts):
                part_of, quarter = e // 4, e % 4
                if quarter == 0:
                    @pl.when(shift == 0)
                    def _():
                        wait_weights(slot, part_of)
                down = ring[slot, part_of, (quarter // 2) * half_rows:(quarter // 2 + 1) * half_rows,
                            pl.ds(pl.multiple_of((quarter % 2) * wcols + shift, bcols), bcols)]
                rows_out = jnp.dot(xs[e, :, :ffn], down, preferred_element_type=F32).astype(BF16)
                for b in range(groups):
                    ybuf[b, e * CAP:(e + 1) * CAP, :] = rows_out[b * CAP:(b + 1) * CAP, :]

        if follow:
            @pl.when(c == per - 1)
            def _():
                start_projection(2, slot)

        @pl.when(jnp.logical_and(c >= 1, c <= blocks))
        def _():
            relay_pair(c - 1)

        @pl.when(c < blocks)
        def _():
            for m in range(chips):
                for k in range(2):
                    sums = jnp.dot(terms[2 * m + k], ybuf[2 * m + k], preferred_element_type=F32)
                    sums = sums[:rows] + sums[rows:2 * rows] + sums[2 * rows:]
                    for s in range(2):
                        part[lax.rem(c, 2), k, s, m] = sums[:, s * sub:(s + 1) * sub]
            pair_copy(c).start()

        @pl.when(jnp.logical_and(c >= MID, c < blocks + MID))
        def _():
            relay_first(c - MID)

        @pl.when(c >= LAG)
        def _():
            finish(c - LAG)
        return carry

    lax.fori_loop(0, blocks + LAG, block_step, 0)
    for copy in gates + ahead + passed:
        copy.wait_send()
    for r in (1, 2):
        for k in range(2):
            across(r, k).wait_send()
    for c in range(blocks):
        for s in range(2):
            for k in range(2):
                first_copy(c, s, k).wait_send()
            second_copy(c, s).wait_send()
    if follow:
        for copy in late:
            copy.wait()
        heads = dim // 128
        at_rows = pl.ds(0, rows)
        xall[at_rows, :] = rms_rows(out_ref[...].astype(F32), attn_gain[layer + 1:layer + 2, :]).astype(BF16)
        cos, sin = rotary(angle, pos_ref, rows, 128)
        leaving = []
        for which in range(3):
            slot = (pairs + which) % SLOTS
            for j in range(2):
                wait_weights(slot, j)
                for n in range(0, ffn, ACOLS):
                    values = jnp.dot(xall[at_rows, :], ring[slot, j, :, n:n + ACOLS], preferred_element_type=F32)
                    if which == 2:
                        xs[which, at_rows, j * ffn + n:j * ffn + n + ACOLS] = values.astype(BF16)
                        continue
                    for i in range(ACOLS // 128):
                        h = (j * ffn + n) // 128 + i
                        step1[h // 4, h // 2 % 2, h % 2] = values[:, i * 128:(i + 1) * 128]
            if which < 2:
                gain_ref = (q_gain, k_gain)[which]
                square = sum(step1[h // 4, h // 2 % 2, h % 2] ** 2 for h in range(heads))
                inv_rms = lax.rsqrt(jnp.sum(square, axis=-1, keepdims=True) / dim + RMS_EPS)
                for h in range(heads):
                    cols = slice(h * 128, (h + 1) * 128)
                    turned = step1[h // 4, h // 2 % 2, h % 2] * inv_rms * gain_ref[layer + 1:layer + 2, cols]
                    turned = turned * cos + pltpu.roll(turned, 64, 1) * sin
                    xs[which, at_rows, cols] = turned.astype(BF16)
            leaving.append(pltpu.make_async_copy(xs.at[which, at_rows], qkv_out.at[which], qsem.at[4 + which]))
            if which:
                leaving[which - 1].start()
    if follow:
        leaving[2].start()
    if follow:
        for copy in leaving:
            copy.wait()


def moe(layer, x1, mlp_gain, ids, router_t, wg, wu, wd, groups, follow):
    rows, dim = x1.shape
    experts, _, ffn = wg.shape
    slots = CAP * groups
    blocks = 8
    bcols = dim // blocks
    chips = groups // 2
    dma = pltpu.SemaphoreType.DMA
    return pl.pallas_call(
        functools.partial(moe_kernel, layer, bool(follow)),
        name="moe",
        out_shape=(jax.ShapeDtypeStruct((rows, dim), BF16),) + ((jax.ShapeDtypeStruct((3, rows, dim), BF16),) if follow else ()),
        in_specs=[ANY] * (7 + len(follow)),
        out_specs=(VMEM, ANY) if follow else (VMEM,),
        scratch_shapes=[
            *([pltpu.SMEM(follow[0].shape, follow[0].dtype), *[pltpu.VMEM(a.shape, a.dtype) for a in follow[1:4]],
               pltpu.VMEM((rows, 128), F32), dma((7,))] if follow else []),
            *[pltpu.VMEM(a.shape, a.dtype) for a in (x1, mlp_gain, ids, router_t)],
            pltpu.VMEM((router_t.shape[0], 128), F32),
            pltpu.VMEM((SLOTS, 2, dim, ffn), BF16),
            pltpu.VMEM((rows * groups, dim), BF16),
            pltpu.VMEM((experts + 1, slots, dim), BF16),
            pltpu.VMEM((groups, experts * CAP, bcols), BF16),
            pltpu.VMEM((chips, 2 * experts * CAP, 2 * rows), BF16),
            pltpu.VMEM((groups, 3 * rows, experts * CAP), BF16),
            pltpu.VMEM((2, 2, 2, chips, rows, bcols // 2), F32),
            pltpu.VMEM((blocks, 2, chips, rows, bcols // 2), F32),
            pltpu.VMEM((blocks, 2, 2, rows, bcols // 2), F32),
            pltpu.VMEM((blocks, 2, rows, bcols // 2), F32),
            pltpu.VMEM((groups, experts, 2 * rows), F32),
            dma((4,)), dma((SLOTS, 2)),
            dma((2, 2)), dma((2, 2)), dma((2,)), dma((2,)), dma((4, 2)), dma((4, 2)), dma((8,)), dma((8,)),
            dma((blocks,)), dma((blocks,)), dma((blocks, 2, 2)), dma((blocks, 2, 2)), dma((blocks, 2)), dma((blocks, 2)),
        ],
        compiler_params=pltpu.CompilerParams(collective_id=layer, has_side_effects=True, vmem_limit_bytes=67043328),
    )(x1, mlp_gain, ids, router_t, wg, wu, wd, *follow)


def solution(mesh):
    groups = mesh.shape['ep']
    batch_axes = ('dp', 'ep')

    def device_step(hidden, positions, expert_ids, k_cache, v_cache, w_query, w_key, w_value, w_out, attn_gain, q_gain, k_gain, mlp_gain, w_router, w_gate, w_up, w_down):
        ids = jnp.transpose(expert_ids, (0, 2, 1))
        router_t = w_router.T
        caches = None
        ready = ()
        for layer in range(expert_ids.shape[0]):
            x1, k_new, v_new = attention(layer, positions, hidden, attn_gain, q_gain, k_gain,
                                         w_query, w_key, w_value, w_out, k_cache, v_cache, caches, ready)
            caches = (k_new, v_new)
            follow = () if layer + 1 == expert_ids.shape[0] else (positions, attn_gain, q_gain, k_gain, w_query, w_key, w_value)
            hidden, *ready = moe(layer, x1, mlp_gain, ids, router_t, w_gate, w_up, w_down, groups, follow)
        return hidden, caches[0], caches[1]

    row_spec = P(batch_axes, None)
    cache_spec = P(None, batch_axes, None, None, None)
    full_spec = P()
    expert_spec = P('ep', None, None)
    in_specs = (row_spec, P(batch_axes), P(None, batch_axes, None), cache_spec, cache_spec, full_spec, full_spec, full_spec, full_spec, full_spec, full_spec, full_spec, full_spec, full_spec, expert_spec, expert_spec, expert_spec)
    return jax.shard_map(device_step, mesh=mesh, in_specs=in_specs, out_specs=(row_spec, cache_spec, cache_spec), check_vma=False)
```
